256 devices in a mesh: dp: 8 (over z), mp: 32 (over y, x, core).
Axes of the slice: x: 4, y: 4, z: 8, core: 2. Of those that a mesh axis runs over, the one named last changes fastest.
Arguments:
- behaviors: bfloat16 [64, 2048, 1024], P('dp', 'mp'), may hold values from -8 to 8
- candidates: bfloat16 [64, 2048, 128], P('dp', 'mp'), may hold values from -12 to 12
- lengths: int32 [64], P('dp'), may hold values from 128 to 1024
- bilinear: bfloat16 [2048, 2048], P('mp'), may hold values from -1 to 2
- norm_gain: float32 [2048], replicated, may hold values from 0.1 to 1.9
- w_gate: bfloat16 [2048, 8192], P('dp', 'mp'), may hold values from -0.125 to 0.125
- w_up: bfloat16 [2048, 8192], P('dp', 'mp'), may hold values from -0.125 to 0.125
- w_down: bfloat16 [8192, 2048], P('mp', 'dp'), may hold values from -0.0625 to 0.0625
Outputs:
- interest: bfloat16 [64, 2048, 128], P('dp', 'mp')
The draws below stay inside these ranges and needn't reach their ends.
All inputs are finite; a program needn't handle non-finite values.
Results may differ from the reference program's by a relative error of at most 0.015.
Values may be sent and summed in bfloat16 or wider, within the bound.
A program may use at most 64 MiB of HBM per device.

```python
import math
import jax
import jax.numpy as jnp
from jax import lax

D = 2048
FF = 8192
L = 1024
C = 128
USERS = 64
N_MP = 32


def base_behaviors(key):
    first_key = jax.random.fold_in(jax.random.fold_in(key, 7), 0)
    bulk = jnp.clip(jax.random.normal(first_key, (USERS, D, L), jnp.float32), -6.0, 6.0)
    return bulk


def draw_behaviors(key, part):
    return base_behaviors(key).astype(jnp.bfloat16)


def draw_candidates(key, part):
    cand_key = jax.random.fold_in(jax.random.fold_in(key, 13), 0)
    cand = jnp.clip(jax.random.normal(cand_key, (USERS, D, C), jnp.float32), -6.0, 6.0)
    return cand.astype(jnp.bfloat16)


def draw_bilinear(key, part):
    noise = jnp.clip(jax.random.normal(jax.random.fold_in(key, 21), (D, D), jnp.float32), -6.0, 6.0)
    return (jnp.eye(D, dtype=jnp.float32) + noise * (0.7 / jnp.sqrt(jnp.float32(D)))).astype(jnp.bfloat16)


def with_ends(drawn, key, low, high):
    shape = drawn.shape
    place = [jax.random.randint(jax.random.fold_in(key, axis), (), 0, shape[axis]) for axis in range(len(shape))]
    drawn = drawn.at[tuple(place)].set(low)
    longest = shape.index(max(shape))
    place[longest] = (place[longest] + 1) % shape[longest]
    return drawn.at[tuple(place)].set(high)


def level_of(rng, extent, shards, smallest, largest):
    factor_of, own = 1.0, jax.random.fold_in(rng, 6)
    for position, blocks in shards:
        heights = jnp.exp(jax.random.uniform(jax.random.fold_in(own, position), (blocks,), jnp.float32, smallest / len(shards), largest / len(shards)))
        factor_of = factor_of * jnp.repeat(heights, extent[position] // blocks).reshape([-1 if axis == position else 1 for axis in range(len(extent))])
    return factor_of


def centred(own_key, extent, width, most, cuts=(), kind=jnp.bfloat16):
    array = jax.random.normal(own_key, extent, jnp.float32) * width
    if len(cuts) > 0:
        array = level_of(own_key, extent, cuts, -0.22, 0.18) * array
    return jnp.clip(array, min=-most, max=most).astype(kind)


def setup_inputs(seed: int = 0) -> dict:
    splits = jax.random.split(jax.random.key(seed), 9)
    behaviors = draw_behaviors(jax.random.fold_in(splits[8], 71), 0)
    candidates = draw_candidates(jax.random.fold_in(splits[8], 71), 0)
    lengths = with_ends(jax.random.randint(splits[2], (USERS,), L // 8, L + 1), jax.random.fold_in(splits[2], 1), L // 8, L).astype(jnp.int32)
    bilinear = draw_bilinear(jax.random.fold_in(splits[8], 71), 0)
    norm_gain = jnp.clip(1.0 + 0.18 * jax.random.normal(splits[4], (D,), jnp.float32), 0.1, 1.9)
    w_gate = centred(splits[5], (D, FF), D ** -0.5, 0.125, ((0, 8), (1, 32)))
    w_up = centred(splits[6], (D, FF), D ** -0.5, 0.125, ((0, 8), (1, 32)))
    w_down = centred(splits[7], (FF, D), FF ** -0.5, 0.0625, ((0, 32), (1, 8)))
    return dict(behaviors=behaviors, candidates=candidates, lengths=lengths, bilinear=bilinear, norm_gain=norm_gain, w_gate=w_gate, w_up=w_up, w_down=w_down)


def one_user(items):
    query, behavior, length = items
    scores = jnp.dot(query.T, behavior, preferred_element_type=jnp.float32) * (1.0 / math.sqrt(D))
    live = lax.broadcasted_iota(jnp.int32, (1, L), 1) < length
    masked = jnp.where(live, scores, -1e+30)
    highest = lax.optimization_barrier(jnp.max(masked, axis=-1, keepdims=True))
    expons = jnp.where(live, jnp.exp(masked - highest), 0.0)
    probs = (expons / lax.optimization_barrier(jnp.sum(expons, axis=-1, keepdims=True))).astype(jnp.bfloat16)
    return jnp.dot(behavior, probs.T, preferred_element_type=jnp.float32).astype(jnp.bfloat16)

def reference(behaviors, candidates, lengths, bilinear, norm_gain, w_gate, w_up, w_down):
    query = jnp.einsum('ek,ukc->uec', bilinear.astype(jnp.float32), candidates.astype(jnp.float32), precision=lax.Precision.HIGHEST)
    query = query.astype(jnp.bfloat16)
    pooled = lax.map(one_user, (query, behaviors, lengths))
    values = pooled.astype(jnp.float32)
    square_mean = lax.optimization_barrier(jnp.mean(values * values, axis=1, keepdims=True))
    normed = (values * lax.rsqrt(square_mean + 1e-06) * norm_gain[None, :, None]).astype(jnp.bfloat16)
    flat = jnp.transpose(normed, (0, 2, 1)).reshape(-1, D)
    gate = jnp.dot(flat, w_gate, preferred_element_type=jnp.float32)
    upward = jnp.dot(flat, w_up, preferred_element_type=jnp.float32)
    hidden = (jax.nn.silu(gate) * upward).astype(jnp.bfloat16)
    group_width = FF // N_MP
    hidden_groups = jnp.transpose(hidden.reshape(hidden.shape[0], N_MP, group_width), (1, 0, 2))
    down_groups = w_down.reshape(N_MP, group_width, D)

    def add_group(total, items):
        hidden_part, down_part = items
        part = jnp.dot(hidden_part, down_part, preferred_element_type=jnp.float32).astype(jnp.bfloat16)
        return (total + part.astype(jnp.float32), None)
    start_total = jnp.zeros((hidden.shape[0], D), jnp.float32)
    total, _ = lax.scan(add_group, start_total, (hidden_groups, down_groups))
    interest = total.astype(jnp.bfloat16)
    return jnp.transpose(interest.reshape(USERS, C, D), (0, 2, 1))
```

```python
import math

import jax
import jax.numpy as jnp
from jax import lax
from jax.experimental import pallas as pl
from jax.experimental.pallas import tpu as pltpu
from jax.sharding import Mesh
from jax.sharding import PartitionSpec as P

MP = ("mp_0", "mp_1", "mp_2")
MESH = pl.DeviceIdType.MESH
BF = jnp.bfloat16
F32 = jnp.float32
USERS_HERE = 8
CANDS = 128
WIDTH = 2048
BEHAVIORS = 1024
TOKENS = USERS_HERE * CANDS
FEATS = 64
UNITS = 256
N_SEMS = 180


class Torus:
    def __init__(self, send_sem, recv_sem):
        self.z = lax.axis_index("dp")
        self.y = lax.axis_index("mp_0")
        self.x = lax.axis_index("mp_1")
        self.c = lax.axis_index("mp_2")
        self.a = self.x + self.c * (self.y - self.x)
        self.b = self.y + self.c * (self.x - self.y)
        self.send_sem, self.recv_sem = send_sem, recv_sem
        self.copies = []

    def dev_a(self, d):
        c = self.c
        return (self.z, lax.rem(self.y + c * d + 4, 4), lax.rem(self.x + (1 - c) * d + 4, 4), c)

    def dev_b(self, d):
        c = self.c
        return (self.z, lax.rem(self.y + (1 - c) * d + 4, 4), lax.rem(self.x + c * d + 4, 4), c)

    def dev_z(self, d):
        return (lax.rem(self.z + d + 8, 8), self.y, self.x, self.c)

    def partner(self):
        return (self.z, self.y, self.x, 1 - self.c)

    def send(self, src, dst, dev):
        i = len(self.copies)
        copy = pltpu.make_async_remote_copy(
            src_ref=src,
            dst_ref=dst,
            send_sem=self.send_sem.at[i],
            recv_sem=self.recv_sem.at[i],
            device_id=dev,
            device_id_type=MESH,
        )
        copy.start()
        self.copies.append(copy)
        return copy

    def finish(self):
        for copy in self.copies:
            copy.wait_send()

    def barrier(self):
        sem = pltpu.get_barrier_semaphore()
        peers = [
            self.dev_a(1),
            self.dev_a(-1),
            self.dev_b(1),
            self.dev_b(-1),
            self.dev_z(1),
            self.dev_z(-1),
            self.partner(),
        ]
        for dev in peers:
            pl.semaphore_signal(sem, inc=1, device_id=dev, device_id_type=MESH)
        pl.semaphore_wait(sem, len(peers))


def all_gather(t, slot, half):
    def at(da, db):
        return lax.rem(t.a + da + 4, 4), lax.rem(t.b + db + 4, 4)

    def whole(da, db, dev):
        ref = slot(*at(da, db))
        return t.send(ref, ref, dev)

    def part(da, db, h, dev):
        ref = half(*at(da, db), h)
        return t.send(ref, ref, dev)

    ap, am, bp, bm = t.dev_a(1), t.dev_a(-1), t.dev_b(1), t.dev_b(-1)
    twin = t.partner()
    twins = []
    first_p = whole(0, 0, ap)
    first_m = whole(0, 0, am)
    from_m, from_p = {}, {}
    from_m[0] = whole(0, 0, bp)
    from_p[0] = whole(0, 0, bm)
    twins.append(whole(0, 0, twin))
    first_p.wait_recv()
    far_0 = part(-1, 0, 0, ap)
    from_m[-1] = whole(-1, 0, bp)
    from_p[-1] = whole(-1, 0, bm)
    twins.append(whole(-1, 0, twin))
    first_m.wait_recv()
    far_1 = part(1, 0, 1, am)
    from_m[1] = whole(1, 0, bp)
    from_p[1] = whole(1, 0, bm)
    twins.append(whole(1, 0, twin))
    ends = {}

    def pass_on(q):
        from_m[q].wait_recv()
        e0 = part(q, -1, 0, bp)
        twins.append(whole(q, -1, twin))
        from_p[q].wait_recv()
        e1 = part(q, 1, 1, bm)
        twins.append(whole(q, 1, twin))
        ends[q] = (e0, e1)

    pass_on(0)
    far_0.wait_recv()
    far_1.wait_recv()
    from_m[2] = whole(2, 0, bp)
    from_p[2] = whole(2, 0, bm)
    twins.append(whole(2, 0, twin))
    for q in (-1, 1, 2):
        pass_on(q)
    for q in (0, -1, 1, 2):
        for e in ends[q]:
            e.wait_recv()
        twins.append(whole(q, 2, twin))
    for copy in twins:
        copy.wait_recv()


def ring_sum(t, p, plus, minus, terms, tx, rx):
    def g(d):
        return lax.rem(p + d + 4, 4)

    def emit(i, value, dev):
        tx[i] = value.astype(BF)
        return t.send(tx.at[i], rx.at[i], dev)

    c0 = emit(0, terms[g(2), 0], plus)
    c1 = emit(1, terms[g(2), 1], minus)
    c2 = emit(2, terms[g(1), 1], plus)
    c3 = emit(3, terms[g(-1), 0], minus)
    c0.wait_recv()
    c4 = emit(4, terms[g(1), 0] + rx[0].astype(F32), plus)
    c1.wait_recv()
    c5 = emit(5, terms[g(-1), 1] + rx[1].astype(F32), minus)
    c3.wait_recv()
    c2.wait_recv()
    c4.wait_recv()
    low = terms[p, 0] + rx[4].astype(F32) + rx[3].astype(F32)
    c5.wait_recv()
    high = terms[p, 1] + rx[2].astype(F32) + rx[5].astype(F32)
    return low, high


def reduce_scatter(t, term, twin_tx, twin_rx, terms, tx, rx, terms_2, tx_2, rx_2):
    other = 1 - t.c
    twins = []
    for d in (2, 1, -1, 0):
        g = lax.rem(t.a + d + 4, 4)
        twin_tx[g] = term(other, g).astype(BF)
        twins.append(t.send(twin_tx.at[g], twin_rx.at[g], t.partner()))
    rows = terms.shape[2]
    order = [lax.rem(t.b + d + 4, 4) for d in (2, 1, -1, 0)]
    for g in order:
        own = term(t.c, g)
        terms[g, 0] = own[:rows]
        terms[g, 1] = own[rows:]
    for copy, g in zip(twins, order):
        copy.wait_recv()
        terms[g, 0] += twin_rx[g, :rows].astype(F32)
        terms[g, 1] += twin_rx[g, rows:].astype(F32)
    low, high = ring_sum(t, t.b, t.dev_b(1), t.dev_b(-1), terms, tx, rx)
    n = terms_2.shape[2]
    for i, part in enumerate((low, high)):
        for j in range(2):
            for h in range(2):
                at = (2 * j + h) * n
                terms_2[2 * i + j, h] = part[at : at + n]
    return ring_sum(t, t.a, t.dev_a(1), t.dev_a(-1), terms_2, tx_2, rx_2)


def dot(a, b, dims=((1,), (0,))):
    return lax.dot_general(a, b, (dims, ((), ())), preferred_element_type=F32)


def kernel(
    cand,
    behaviors,
    lengths,
    bilinear,
    gain,
    w_gate,
    w_up,
    w_down,
    out,
    weights,
    cands,
    query,
    twin_tx,
    twin_rx,
    terms,
    tx,
    rx,
    terms_2,
    tx_2,
    rx_2,
    probs,
    pooled,
    hidden,
    out_twin_tx,
    out_twin_rx,
    out_terms,
    out_tx,
    out_rx,
    out_terms_2,
    out_tx_2,
    out_rx_2,
    send_sem,
    recv_sem,
):
    t = Torus(send_sem, recv_sem)
    t.barrier()
    mine = (t.y * 4 + t.x) * 2 + t.c

    own_gain = gain[pl.ds(t.z, 1), :]
    for i, w in enumerate((w_gate, w_up)):
        weights[t.z, pl.ds(i * UNITS, UNITS), :] = (w[...].astype(F32).T * own_gain).astype(BF)
    weights[t.z, pl.ds(2 * UNITS, UNITS), :] = w_down[...].astype(F32).T.astype(BF)

    def zat(d):
        return lax.rem(t.z + d + 8, 8)

    def pass_weights(d):
        up = t.send(weights.at[zat(1 - d)], weights.at[zat(1 - d)], t.dev_z(1))
        down = t.send(weights.at[zat(d - 1)], weights.at[zat(d - 1)], t.dev_z(-1))
        return up, down

    def feature_slot(buf):
        def chip(a, b):
            y = b + t.c * (a - b)
            x = a + t.c * (b - a)
            return (y * 4 + x) * 2 + t.c

        return (
            lambda a, b: buf.at[chip(a, b)],
            lambda a, b, h: buf.at[chip(a, b), pl.ds(h * (FEATS // 2), FEATS // 2), :],
        )

    for u in range(USERS_HERE):
        cands[mine, :, pl.ds(u * CANDS, CANDS)] = cand[u]
    w_hop = pass_weights(1)
    all_gather(t, *feature_slot(cands))

    q = dot(bilinear[...], cands[...].reshape(WIDTH, TOKENS)).astype(BF)
    for u in range(USERS_HERE):
        query[u] = q[:, u * CANDS : (u + 1) * CANDS]
    for copy in w_hop:
        copy.wait_recv()
    w_hop = pass_weights(2)

    def scores(core, group):
        u = core * 4 + group
        return dot(query[u], behaviors[u], ((0,), (0,)))

    low, high = reduce_scatter(
        t, scores, twin_tx, twin_rx, terms, tx, rx, terms_2, tx_2, rx_2
    )
    for copy in w_hop:
        copy.wait_recv()
    w_hop = pass_weights(3)
    length = lengths[t.c * 4 + t.b]
    block = t.c * 16 + t.b * 4 + t.a
    for i, part in enumerate((low, high)):
        s = part * (1.0 / math.sqrt(WIDTH))
        live = lax.broadcasted_iota(jnp.int32, s.shape, 1) < length
        s = jnp.where(live, s, -1e30)
        e = jnp.where(live, jnp.exp(s - jnp.max(s, axis=1, keepdims=True)), 0.0)
        e = e / jnp.sum(e, axis=1, keepdims=True)
        n = s.shape[0]
        probs[block, pl.ds(i * n, n), :] = e.astype(BF)

    all_gather(
        t,
        lambda a, b: probs.at[t.c * 16 + b * 4 + a],
        lambda a, b, h: probs.at[t.c * 16 + b * 4 + a, pl.ds(h * 16, 16), :],
    )
    for copy in w_hop:
        copy.wait_recv()
    far_w = zat(4)
    last_up = t.send(
        weights.at[zat(-3), pl.ds(0, 384)], weights.at[zat(-3), pl.ds(0, 384)], t.dev_z(1)
    )
    last_down = t.send(
        weights.at[zat(3), pl.ds(384, 384)], weights.at[zat(3), pl.ds(384, 384)], t.dev_z(-1)
    )
    for u in range(USERS_HERE):
        p = probs[pl.ds(4 * u, 4)].reshape(CANDS, BEHAVIORS)
        pooled[mine, :, pl.ds(u * CANDS, CANDS)] = dot(
            behaviors[u], p, ((1,), (1,))
        ).astype(BF)
    all_gather(t, *feature_slot(pooled))
    last_up.wait_recv()
    last_down.wait_recv()

    n = 256
    for i in range(TOKENS // n):
        lanes = pl.ds(i * n, n)
        acc = jnp.zeros((2 * UNITS, n), F32)
        squares = jnp.zeros((1, n), F32)
        for k in range(8):
            x = pooled[pl.ds(4 * k, 4), :, lanes].reshape(256, n)
            acc += dot(weights[k, pl.ds(0, 2 * UNITS), :], x)
            v = x.astype(F32)
            squares += jnp.sum(v * v, axis=0, keepdims=True)
        acc = acc * lax.rsqrt(squares * (1.0 / WIDTH) + 1e-6)
        gate, upward = acc[:UNITS], acc[UNITS:]
        hidden[:, lanes] = (gate / (1.0 + jnp.exp(-gate)) * upward).astype(BF)

    def outputs(core, group):
        parts = []
        for i in range(4):
            y = group + core * (i - group)
            x = i + core * (group - i)
            m = (y * 4 + x) * 2 + core
            at = 2 * UNITS + lax.rem(m, 4) * FEATS
            parts.append(weights[m // 4, pl.ds(pl.multiple_of(at, FEATS), FEATS), :])
        return dot(jnp.concatenate(parts, axis=0), hidden[...])

    low, high = reduce_scatter(
        t,
        outputs,
        out_twin_tx,
        out_twin_rx,
        out_terms,
        out_tx,
        out_rx,
        out_terms_2,
        out_tx_2,
        out_rx_2,
    )
    n = FEATS // 2
    for u in range(USERS_HERE):
        out[u, pl.ds(0, n), :] = low[:, u * CANDS : (u + 1) * CANDS].astype(BF)
        out[u, pl.ds(n, n), :] = high[:, u * CANDS : (u + 1) * CANDS].astype(BF)
    t.finish()


def shards(behaviors, candidates, lengths, bilinear, norm_gain, w_gate, w_up, w_down):
    vmem = pl.BlockSpec(memory_space=pltpu.VMEM)
    smem = pl.BlockSpec(memory_space=pltpu.SMEM)
    return pl.pallas_call(
        kernel,
        out_shape=jax.ShapeDtypeStruct(candidates.shape, BF),
        in_specs=[vmem, vmem, smem, vmem, vmem, vmem, vmem, vmem],
        out_specs=vmem,
        scratch_shapes=[
            pltpu.VMEM((8, 3 * UNITS, UNITS), BF),
            pltpu.VMEM((32, FEATS, TOKENS), BF),
            pltpu.VMEM((USERS_HERE, FEATS, CANDS), BF),
            pltpu.VMEM((4, CANDS, BEHAVIORS), BF),
            pltpu.VMEM((4, CANDS, BEHAVIORS), BF),
            pltpu.VMEM((4, 2, 64, BEHAVIORS), F32),
            pltpu.VMEM((6, 64, BEHAVIORS), BF),
            pltpu.VMEM((6, 64, BEHAVIORS), BF),
            pltpu.VMEM((4, 2, 16, BEHAVIORS), F32),
            pltpu.VMEM((6, 16, BEHAVIORS), BF),
            pltpu.VMEM((6, 16, BEHAVIORS), BF),
            pltpu.VMEM((32, 32, BEHAVIORS), BF),
            pltpu.VMEM((32, FEATS, TOKENS), BF),
            pltpu.VMEM((UNITS, TOKENS), BF),
            pltpu.VMEM((4, 256, TOKENS), BF),
            pltpu.VMEM((4, 256, TOKENS), BF),
            pltpu.VMEM((4, 2, 128, TOKENS), F32),
            pltpu.VMEM((6, 128, TOKENS), BF),
            pltpu.VMEM((6, 128, TOKENS), BF),
            pltpu.VMEM((4, 2, 32, TOKENS), F32),
            pltpu.VMEM((6, 32, TOKENS), BF),
            pltpu.VMEM((6, 32, TOKENS), BF),
            pltpu.SemaphoreType.DMA((N_SEMS,)),
            pltpu.SemaphoreType.DMA((N_SEMS,)),
        ],
        compiler_params=pltpu.CompilerParams(
            collective_id=0, has_side_effects=True, vmem_limit_bytes=56 * 1024 * 1024
        ),
    )(
        candidates,
        behaviors,
        lengths,
        bilinear,
        norm_gain.reshape(8, 256),
        w_gate,
        w_up,
        w_down,
    )


def solution(mesh):
    finer = Mesh(mesh.devices.reshape(mesh.shape["dp"], 4, 4, 2), ("dp", "mp_0", "mp_1", "mp_2"))
    return jax.shard_map(
        shards,
        mesh=finer,
        in_specs=(
            P("dp", MP, None),
            P("dp", MP, None),
            P("dp"),
            P(MP, None),
            P(),
            P("dp", MP),
            P("dp", MP),
            P(MP, "dp"),
        ),
        out_specs=P("dp", MP, None),
        check_vma=False,
    )
```

```python
import math

import jax
import jax.numpy as jnp
from jax import lax
from jax.experimental import pallas as pl
from jax.experimental.pallas import tpu as pltpu
from jax.sharding import Mesh
from jax.sharding import PartitionSpec as P

MP = ("mp_0", "mp_1", "mp_2")
MESH = pl.DeviceIdType.MESH
BF = jnp.bfloat16
F32 = jnp.float32
USERS_HERE = 8
CANDS = 128
WIDTH = 2048
BEHAVIORS = 1024
CHUNKS = 2
CHUNK_USERS = USERS_HERE // CHUNKS
TOKENS = CHUNK_USERS * CANDS
QUARTER = BEHAVIORS // 4
FEATURES = WIDTH // 4
ROWS = CANDS // CHUNKS
OTHERS = sorted(
    ((dy, dx, dc) for dy in range(4) for dx in range(4) for dc in range(2) if dy + dx + dc),
    key=lambda d: (-min(d[0], 4 - d[0]) - min(d[1], 4 - d[1]), d),
)
LEAD = 0
LAST_HOP = 9
TICK = 2
FEATS = 64
UNITS = 256
N_SEMS = 320


class Torus:
    def __init__(self, send_sem, recv_sem):
        self.z = lax.axis_index("dp")
        self.y = lax.axis_index("mp_0")
        self.x = lax.axis_index("mp_1")
        self.c = lax.axis_index("mp_2")
        self.a = self.x + self.c * (self.y - self.x)
        self.b = self.y + self.c * (self.x - self.y)
        self.me = (self.y * 4 + self.x) * 2 + self.c
        self.user, self.quarter = owned(self.y, self.x, self.c)
        self.send_sem, self.recv_sem = send_sem, recv_sem
        self.copies = []

    def chip(self, a, b):
        return b + self.c * (a - b), a + self.c * (b - a)

    def shifted(self, dy, dx, dc):
        core = 1 - self.c if dc else self.c
        return lax.rem(self.y + dy, 4), lax.rem(self.x + dx, 4), core

    def dev_a(self, d):
        c = self.c
        return (self.z, lax.rem(self.y + c * d + 4, 4), lax.rem(self.x + (1 - c) * d + 4, 4), c)

    def dev_b(self, d):
        c = self.c
        return (self.z, lax.rem(self.y + (1 - c) * d + 4, 4), lax.rem(self.x + c * d + 4, 4), c)

    def dev_z(self, d):
        return (lax.rem(self.z + d + 8, 8), self.y, self.x, self.c)

    def partner(self):
        return (self.z, self.y, self.x, 1 - self.c)

    def send(self, src, dst, dev):
        i = len(self.copies)
        copy = pltpu.make_async_remote_copy(
            src_ref=src,
            dst_ref=dst,
            send_sem=self.send_sem.at[i],
            recv_sem=self.recv_sem.at[i],
            device_id=dev,
            device_id_type=MESH,
        )
        copy.start()
        self.copies.append(copy)
        return copy

    def finish(self):
        for copy in self.copies:
            copy.wait_send()

    def barrier(self):
        sem = pltpu.get_barrier_semaphore()
        peers = [self.dev_z(1), self.dev_z(-1)]
        peers += [(self.z, *self.shifted(*d)) for d in OTHERS]
        for dev in peers:
            pl.semaphore_signal(sem, inc=1, device_id=dev, device_id_type=MESH)
        pl.semaphore_wait(sem, len(peers))


def owned(y, x, core):
    return y * 2 + x // 2, lax.rem(x, 2) * 2 + core


def all_gather(t, slot):
    def whole(da, db, dev):
        ref = slot(lax.rem(t.a + da + 4, 4), lax.rem(t.b + db + 4, 4))
        return t.send(ref, ref, dev)

    twin = t.partner()
    row = {d: whole(0, 0, t.dev_a(d)) for d in (2, 1, -1)}
    column = {(0, d): whole(0, 0, t.dev_b(d)) for d in (2, 1, -1)}
    twins = [whole(0, 0, twin)]
    for q in (-1, 1, 2):
        yield
        row[q].wait_recv()
        for d in (2, 1, -1):
            column[-q, d] = whole(-q, 0, t.dev_b(d))
        twins.append(whole(-q, 0, twin))
    for (q, d), copy in column.items():
        yield
        copy.wait_recv()
        twins.append(whole(q, -d, twin))
    yield
    for copy in twins:
        copy.wait_recv()


def ring_sum(t, p, dev, terms, tx, rx):
    copies = []
    for i, d in enumerate((2, 1, -1)):
        tx[i] = terms[lax.rem(p + d + 4, 4)].astype(tx.dtype)
        copies.append(t.send(tx.at[i], rx.at[i], dev(d)))
    total = terms[p]
    for i in (1, 2, 0):
        yield
        copies[i].wait_recv()
        total += rx[i].astype(F32)
    return total


def reduce_scatter(t, term, twin_tx, twin_rx, terms, tx, rx, terms_2, tx_2, rx_2):
    other = 1 - t.c
    twins = []
    for d in (2, 1, -1, 0):
        g = lax.rem(t.a + d + 4, 4)
        twin_tx[g] = term(other, g).astype(twin_tx.dtype)
        twins.append(t.send(twin_tx.at[g], twin_rx.at[g], t.partner()))
    order = [lax.rem(t.b + d + 4, 4) for d in (2, 1, -1, 0)]
    for g in order:
        terms[g] = term(t.c, g)
    yield
    for copy, g in zip(twins, order):
        copy.wait_recv()
        terms[g] += twin_rx[g].astype(F32)
    total = yield from ring_sum(t, t.b, t.dev_b, terms, tx, rx)
    n = terms_2.shape[1]
    for i in range(4):
        terms_2[i] = total[i * n : (i + 1) * n]
    return (yield from ring_sum(t, t.a, t.dev_a, terms_2, tx_2, rx_2))


def dot(a, b, dims=((1,), (0,))):
    return lax.dot_general(a, b, (dims, ((), ())), preferred_element_type=F32)


class Weights:
    def __init__(self, t, buf):
        self.t, self.buf, self.hops, self.pending, self.ticks = t, buf, 0, (), 0

    def at(self, d):
        return lax.rem(self.t.z + d + 8, 8)

    def wait(self):
        for copy in self.pending:
            copy.wait_recv()
        self.pending = ()

    def late_hop(self):
        self.ticks += 1
        if self.ticks == LAST_HOP:
            self.hop()

    def hop(self):
        self.wait()
        t, d = self.t, self.hops
        self.hops += 1
        up, down = self.buf.at[self.at(-d)], self.buf.at[self.at(d)]
        if d == 3:
            n = self.buf.shape[1] // 2
            up = self.buf.at[self.at(-d), pl.ds(0, n)]
            down = self.buf.at[self.at(d), pl.ds(n, n)]
        self.pending = (t.send(up, up, t.dev_z(1)), t.send(down, down, t.dev_z(-1)))


def together(chains, tick=None, lead=0):
    chains = list(chains)
    ended = object()
    for _ in range(lead):
        next(chains[0])
    while chains:
        for one in list(chains):
            if next(one, ended) is ended:
                chains.remove(one)
        if tick is not None:
            tick()


def attend(t, mem, w):
    u = t.user
    copies = []
    for dy, dx, dc in OTHERS:
        if dc == 0:
            y, x, c = t.shifted(dy, dx, dc)
            copies.append((dy, dx, t.send(mem.query.at[owned(y, x, c)[0]], mem.keys.at[t.me], (t.z, y, x, c))))
    mem.keys[t.me] = mem.query[u]
    twins = [t.send(mem.keys.at[t.me], mem.keys.at[t.me], t.partner())]
    w.hop()
    for dy, dx, copy in reversed(copies):
        copy.wait_recv()
        y, x = lax.rem(t.y - dy + 4, 4), lax.rem(t.x - dx + 4, 4)
        ref = mem.keys.at[(y * 4 + x) * 2 + t.c]
        twins.append(t.send(ref, ref, t.partner()))
    for copy in mem.moved:
        copy.wait_recv()
    mem.own_behaviors.wait()
    for copy in twins:
        copy.wait_recv()
    behaviors = mem.behaviors[...].reshape(WIDTH, QUARTER)
    s = dot(mem.keys[...].reshape(WIDTH, CANDS), behaviors, ((0,), (0,)))
    s = s * (1.0 / math.sqrt(WIDTH))
    at = lax.broadcasted_iota(jnp.int32, s.shape, 1) + t.quarter * QUARTER
    live = at < mem.lengths[u]
    s = jnp.where(live, s, -1e30)
    highest = jnp.max(s, axis=1, keepdims=True)
    e = jnp.where(live, jnp.exp(s - highest), 0.0)
    total = jnp.sum(e, axis=1, keepdims=True)
    some = total > 0.0
    total = jnp.where(some, total, 1.0)
    level = jnp.where(some, highest + jnp.log(total), -1e30)
    level = jnp.broadcast_to(level, (CANDS, 128))
    mem.levels[...] = level
    mem.level_tx[...] = level.T[:8]
    mem.level_copies = [
        t.send(mem.level_tx, mem.level_rx.at[i], dev) for i, (dev, _) in enumerate(owners(t))
    ]
    p = (e / total).astype(BF)
    for i in range(4):
        mem.means[i] = dot(p, mem.behaviors[pl.ds(8 * i, 8)].reshape(FEATURES, QUARTER), ((1,), (1,)))


def owners(t):
    x = t.x + 1 - 2 * lax.rem(t.x, 2)
    result = []
    for xx, c in ((x, 1 - t.c), (x, t.c), (t.x, 1 - t.c)):
        result.append(((t.z, t.y, xx, c), owned(t.y, xx, c)[1]))
    return result


def chain(t, h, mem, w):
    rows = pl.ds(h * ROWS, ROWS)
    copies = []
    for i, (dev, quarter) in enumerate(owners(t)):
        mem.mean_tx[h, i] = mem.means[quarter, rows, :].astype(BF)
        copies.append(t.send(mem.mean_tx.at[h, i], mem.mean_rx.at[h, i], dev))
    yield
    if h == 0:
        for copy in mem.level_copies:
            copy.wait_recv()
        levels = [mem.levels[...]]
        levels += [jnp.broadcast_to(mem.level_rx[i][:1], (128, CANDS)).T for i in range(3)]
        top = jnp.maximum(jnp.maximum(levels[0], levels[1]), jnp.maximum(levels[2], levels[3]))
        shares = [jnp.exp(level - top) for level in levels]
        scale = 1.0 / (shares[0] + shares[1] + shares[2] + shares[3])
        for i in range(4):
            mem.shares[i] = shares[i] * scale

    def share(i):
        return jnp.concatenate([mem.shares[i, rows, :]] * (FEATURES // 128), axis=1)

    total = mem.means[t.quarter, rows, :] * share(0)
    for i in (2, 1, 0):
        copies[i].wait_recv()
        total += mem.mean_rx[h, i].astype(F32) * share(i + 1)
    mem.pooled[h, t.quarter, t.user] = total.astype(BF)

    def pooled_slot(a, b):
        user, quarter = owned(*t.chip(a, b), t.c)
        return mem.pooled.at[h, quarter, user]

    yield from all_gather(t, pooled_slot)
    if h == 0:
        w.wait()

    n = 256
    for i in range(TOKENS // n):
        acc = jnp.zeros((n, 2 * UNITS), F32)
        squares = jnp.zeros((n, 1), F32)
        for k in range(4):
            x = mem.pooled[h, k, pl.ds(4 * i, 4)].reshape(n, FEATURES)
            acc += dot(x, mem.weights[pl.ds(2 * k, 2), :, pl.ds(0, 2 * UNITS)].reshape(FEATURES, 2 * UNITS))
            v = x.astype(F32)
            squares += jnp.sum(v * v, axis=1, keepdims=True)
        acc = acc * lax.rsqrt(squares * (1.0 / WIDTH) + 1e-6)
        gate, upward = acc[:, :UNITS], acc[:, UNITS:]
        value = gate / (1.0 + jnp.exp(-gate)) * upward
        mem.hidden[h, :, pl.ds(i * n, n)] = value.T.astype(BF)
    yield

    def outputs(core, group):
        parts = []
        for i in range(4):
            y = group + core * (i - group)
            x = i + core * (group - i)
            m = (y * 4 + x) * 2 + core
            at = pl.multiple_of(lax.rem(m, 4) * FEATS, FEATS)
            parts.append(mem.weights[m // 4, pl.ds(at, FEATS), pl.ds(2 * UNITS, UNITS)])
        return dot(jnp.concatenate(parts, axis=0), mem.hidden[h])

    total = yield from reduce_scatter(
        t,
        outputs,
        *(ref.at[h] for ref in mem.out_1),
        *(ref.at[h] for ref in mem.out_2),
    )
    mem.result[h] = total


class Memory:
    pass


def kernel(
    cand_in,
    behaviors_in,
    lengths,
    bilinear_in,
    gain,
    w_gate_in,
    w_up_in,
    w_down_in,
    out,
    behaviors,
    bilinear,
    raw_weights,
    weights,
    cands,
    query,
    keys,
    means,
    mean_tx,
    mean_rx,
    levels,
    level_tx,
    level_rx,
    shares,
    pooled,
    hidden,
    result,
    *rest,
):
    send_sem, recv_sem, in_sem = rest[-3:]
    t = Torus(send_sem, recv_sem)
    mem = Memory()
    mem.behaviors, mem.bilinear, mem.weights, mem.cands = behaviors, bilinear, weights, cands
    mem.query, mem.keys, mem.pooled, mem.hidden = query, keys, pooled, hidden
    mem.means, mem.mean_tx, mem.mean_rx, mem.shares = means, mean_tx, mean_rx, shares
    mem.levels, mem.level_tx, mem.level_rx = levels, level_tx, level_rx
    mem.lengths, mem.result = lengths, result
    mem.out_1, mem.out_2 = rest[0:5], rest[5:8]

    started = []

    def fetch(src, dst):
        copy = pltpu.make_async_copy(src, dst, in_sem.at[len(started)])
        copy.start()
        started.append(copy)
        return copy

    cand_copies = [
        fetch(
            cand_in.at[u],
            cands.at[u // CHUNK_USERS, t.me, :, pl.ds(u % CHUNK_USERS * CANDS, CANDS)],
        )
        for u in range(USERS_HERE)
    ]
    weight_copies = [
        fetch(w, raw_weights.at[i]) for i, w in enumerate((w_gate_in, w_up_in, w_down_in))
    ]
    bilinear_copy = fetch(bilinear_in, bilinear)

    def behaviors_of(y, x, core):
        user, quarter = owned(y, x, core)
        at = pl.multiple_of(quarter * QUARTER, QUARTER)
        return behaviors_in.at[user, :, pl.ds(at, QUARTER)]

    mem.own_behaviors = fetch(behaviors_of(t.y, t.x, t.c), behaviors.at[t.me])
    t.barrier()

    to_move = list(OTHERS)
    mem.moved = []

    def move_behaviors(count=TICK):
        for _ in range(min(count, len(to_move))):
            y, x, c = t.shifted(*to_move.pop(0))
            mem.moved.append(t.send(behaviors_of(y, x, c), behaviors.at[t.me], (t.z, y, x, c)))

    def cand_slot(h):
        def slot(a, b):
            y, x = t.chip(a, b)
            return cands.at[h, (y * 4 + x) * 2 + t.c]

        return slot

    w = Weights(t, weights)
    for copy in cand_copies:
        copy.wait()
    gathers = [all_gather(t, cand_slot(h)) for h in range(CHUNKS)]
    for one in gathers:
        next(one)
    move_behaviors()

    own_gain = jnp.broadcast_to(gain[pl.ds(t.z, 1), :], (128, UNITS)).T
    own_gain = jnp.concatenate([own_gain, own_gain], axis=1)
    for i in range(3):
        weight_copies[i].wait()
        v = raw_weights[i].astype(F32)
        v = v * own_gain if i < 2 else v.T
        weights[t.z, :, pl.ds(i * UNITS, UNITS)] = v.astype(BF)
    w.hop()

    together(gathers, move_behaviors)
    move_behaviors(len(to_move))
    bilinear_copy.wait()
    for h in range(CHUNKS):
        q = dot(bilinear[...], cands[h].reshape(WIDTH, TOKENS)).astype(BF)
        for u in range(CHUNK_USERS):
            query[h * CHUNK_USERS + u] = q[:, u * CANDS : (u + 1) * CANDS]
    attend(t, mem, w)
    w.hop()
    together([chain(t, h, mem, w) for h in range(CHUNKS)], w.late_hop, LEAD)
    for u in range(USERS_HERE):
        parts = [result[h, :, pl.ds(u // 2 * 128, 128)] for h in range(CHUNKS)]
        if u % 2 == 0:
            both = jnp.concatenate([part[:, :ROWS] for part in parts], axis=1)
        else:
            both = jnp.concatenate([part[:, ROWS:] for part in parts], axis=1)
        out[u] = both.astype(BF)
    t.finish()


def exchange_buffers(rows, piece, width):
    return (
        pltpu.VMEM((CHUNKS, 4, rows, width), BF),
        pltpu.VMEM((CHUNKS, 4, rows, width), BF),
        pltpu.VMEM((CHUNKS, 4, rows, width), F32),
        pltpu.VMEM((CHUNKS, 3, rows, width), BF),
        pltpu.VMEM((CHUNKS, 3, rows, width), BF),
        pltpu.VMEM((CHUNKS, 4, piece, width), F32),
        pltpu.VMEM((CHUNKS, 3, piece, width), BF),
        pltpu.VMEM((CHUNKS, 3, piece, width), BF),
    )


def shards(behaviors, candidates, lengths, bilinear, norm_gain, w_gate, w_up, w_down):
    vmem = pl.BlockSpec(memory_space=pltpu.VMEM)
    hbm = pl.BlockSpec(memory_space=pl.ANY)
    smem = pl.BlockSpec(memory_space=pltpu.SMEM)
    return pl.pallas_call(
        kernel,
        out_shape=jax.ShapeDtypeStruct(candidates.shape, BF),
        in_specs=[hbm, hbm, smem, hbm, vmem, hbm, hbm, hbm],
        out_specs=vmem,
        scratch_shapes=[
            pltpu.VMEM((32, FEATS, QUARTER), BF),
            pltpu.VMEM(bilinear.shape, BF),
            pltpu.VMEM((3, UNITS, UNITS), BF),
            pltpu.VMEM((8, UNITS, 3 * UNITS), BF),
            pltpu.VMEM((CHUNKS, 32, FEATS, TOKENS), BF),
            pltpu.VMEM((USERS_HERE, FEATS, CANDS), BF),
            pltpu.VMEM((32, FEATS, CANDS), BF),
            pltpu.VMEM((4, CANDS, FEATURES), F32),
            pltpu.VMEM((CHUNKS, 3, ROWS, FEATURES), BF),
            pltpu.VMEM((CHUNKS, 3, ROWS, FEATURES), BF),
            pltpu.VMEM((CANDS, 128), F32),
            pltpu.VMEM((8, CANDS), F32),
            pltpu.VMEM((3, 8, CANDS), F32),
            pltpu.VMEM((4, CANDS, 128), F32),
            pltpu.VMEM((CHUNKS, 4, USERS_HERE, ROWS, FEATURES), BF),
            pltpu.VMEM((CHUNKS, UNITS, TOKENS), BF),
            pltpu.VMEM((CHUNKS, FEATS, TOKENS), F32),
            *exchange_buffers(256, FEATS, TOKENS),
            pltpu.SemaphoreType.DMA((N_SEMS,)),
            pltpu.SemaphoreType.DMA((N_SEMS,)),
            pltpu.SemaphoreType.DMA((16,)),
        ],
        compiler_params=pltpu.CompilerParams(
            collective_id=0, has_side_effects=True, vmem_limit_bytes=56 * 1024 * 1024
        ),
    )(
        candidates,
        behaviors,
        lengths,
        bilinear,
        norm_gain.reshape(8, 256),
        w_gate,
        w_up,
        w_down,
    )


def solution(mesh):
    finer = Mesh(mesh.devices.reshape(mesh.shape["dp"], 4, 4, 2), ("dp", "mp_0", "mp_1", "mp_2"))
    return jax.shard_map(
        shards,
        mesh=finer,
        in_specs=(
            P("dp", MP, None),
            P("dp", MP, None),
            P("dp"),
            P(MP, None),
            P(),
            P("dp", MP),
            P("dp", MP),
            P(MP, "dp"),
        ),
        out_specs=P("dp", MP, None),
        check_vma=False,
    )
```

```python
import math

import jax
import jax.numpy as jnp
from jax import lax
from jax.experimental import pallas as pl
from jax.experimental.pallas import tpu as pltpu
from jax.sharding import Mesh
from jax.sharding import PartitionSpec as P

MP = ("mp_0", "mp_1", "mp_2")
MESH = pl.DeviceIdType.MESH
BF = jnp.bfloat16
F32 = jnp.float32
USERS_HERE = 8
CANDS = 128
WIDTH = 2048
BEHAVIORS = 1024
CHUNKS = 2
CHUNK_USERS = USERS_HERE // CHUNKS
TOKENS = CHUNK_USERS * CANDS
QUARTER = BEHAVIORS // 4
FEATURES = WIDTH // 4
ROWS = CANDS // CHUNKS
OTHERS = sorted(
    ((dy, dx, dc) for dy in range(4) for dx in range(4) for dc in range(2) if dy + dx + dc),
    key=lambda d: (-min(d[0], 4 - d[0]) - min(d[1], 4 - d[1]), d),
)
LEAD = 0
SECOND_HOP = 8
LAST_HOP = 6
MOVE_AT = 3
MOVE = 20
CAND_HALVES = 32
MEAN_HALVES = None
FEATS = 64
UNITS = 256
N_SEMS = 320


class Torus:
    def __init__(self, send_sem, recv_sem):
        self.z = lax.axis_index("dp")
        self.y = lax.axis_index("mp_0")
        self.x = lax.axis_index("mp_1")
        self.c = lax.axis_index("mp_2")
        self.a = self.x + self.c * (self.y - self.x)
        self.b = self.y + self.c * (self.x - self.y)
        self.me = (self.y * 4 + self.x) * 2 + self.c
        self.user, self.quarter = owned(self.y, self.x, self.c)
        self.send_sem, self.recv_sem = send_sem, recv_sem
        self.copies = []

    def chip(self, a, b):
        return b + self.c * (a - b), a + self.c * (b - a)

    def shifted(self, dy, dx, dc):
        core = 1 - self.c if dc else self.c
        return lax.rem(self.y + dy, 4), lax.rem(self.x + dx, 4), core

    def dev_a(self, d):
        c = self.c
        return (self.z, lax.rem(self.y + c * d + 4, 4), lax.rem(self.x + (1 - c) * d + 4, 4), c)

    def dev_b(self, d):
        c = self.c
        return (self.z, lax.rem(self.y + (1 - c) * d + 4, 4), lax.rem(self.x + c * d + 4, 4), c)

    def dev_z(self, d):
        return (lax.rem(self.z + d + 8, 8), self.y, self.x, self.c)

    def partner(self):
        return (self.z, self.y, self.x, 1 - self.c)

    def send(self, src, dst, dev):
        i = len(self.copies)
        copy = pltpu.make_async_remote_copy(
            src_ref=src,
            dst_ref=dst,
            send_sem=self.send_sem.at[i],
            recv_sem=self.recv_sem.at[i],
            device_id=dev,
            device_id_type=MESH,
        )
        copy.start()
        self.copies.append(copy)
        return copy

    def finish(self):
        for copy in self.copies:
            copy.wait_send()

    def barrier(self):
        sem = pltpu.get_barrier_semaphore()
        peers = [self.dev_z(1), self.dev_z(-1)]
        peers += [(self.z, *self.shifted(*d)) for d in OTHERS]
        for dev in peers:
            pl.semaphore_signal(sem, inc=1, device_id=dev, device_id_type=MESH)
        pl.semaphore_wait(sem, len(peers))


def owned(y, x, core):
    return y * 2 + x // 2, lax.rem(x, 2) * 2 + core


def all_gather(t, slot, halves=None):
    def block(da, db):
        return slot(lax.rem(t.a + da + 4, 4), lax.rem(t.b + db + 4, 4))

    def whole(da, db, dev):
        ref = block(da, db)
        return t.send(ref, ref, dev)

    def part(da, db, h, dev):
        ref = block(da, db).at[pl.ds(h * halves, halves), :]
        return t.send(ref, ref, dev)

    twin = t.partner()
    far = (2, 1, -1) if halves is None else (1, -1)
    row = {d: whole(0, 0, t.dev_a(d)) for d in (2, 1, -1)}
    column = {(0, d): whole(0, 0, t.dev_b(d)) for d in far}
    twins = [whole(0, 0, twin)]
    for q in (-1, 1, 2):
        yield
        row[q].wait_recv()
        for d in far:
            column[-q, d] = whole(-q, 0, t.dev_b(d))
        twins.append(whole(-q, 0, twin))
    ends = {}
    for (q, d), copy in column.items():
        yield
        copy.wait_recv()
        if halves is not None:
            ends.setdefault(q, []).append(part(q, -d, 0 if d == 1 else 1, t.dev_b(d)))
        twins.append(whole(q, -d, twin))
    for q, copies in ends.items():
        yield
        for copy in copies:
            copy.wait_recv()
        twins.append(whole(q, 2, twin))
    yield
    for copy in twins:
        copy.wait_recv()


def ring_sum(t, p, dev, terms, tx, rx):
    copies = []
    for i, d in enumerate((2, 1, -1)):
        tx[i] = terms[lax.rem(p + d + 4, 4)].astype(tx.dtype)
        copies.append(t.send(tx.at[i], rx.at[i], dev(d)))
    total = terms[p]
    for i in (1, 2, 0):
        yield
        copies[i].wait_recv()
        total += rx[i].astype(F32)
    return total


def reduce_scatter(t, term, twin_tx, twin_rx, terms, tx, rx, terms_2, tx_2, rx_2):
    other = 1 - t.c
    twins = []
    for d in (2, 1, -1, 0):
        g = lax.rem(t.a + d + 4, 4)
        twin_tx[g] = term(other, g).astype(twin_tx.dtype)
        twins.append(t.send(twin_tx.at[g], twin_rx.at[g], t.partner()))
    order = [lax.rem(t.b + d + 4, 4) for d in (2, 1, -1, 0)]
    for g in order:
        terms[g] = term(t.c, g)
    yield
    for copy, g in zip(twins, order):
        copy.wait_recv()
        terms[g] += twin_rx[g].astype(F32)
    total = yield from ring_sum(t, t.b, t.dev_b, terms, tx, rx)
    n = terms_2.shape[1]
    for i in range(4):
        terms_2[i] = total[i * n : (i + 1) * n]
    return (yield from ring_sum(t, t.a, t.dev_a, terms_2, tx_2, rx_2))


def dot(a, b, dims=((1,), (0,))):
    return lax.dot_general(a, b, (dims, ((), ())), preferred_element_type=F32)


class Weights:
    def __init__(self, t, buf):
        self.t, self.buf, self.hops, self.pending, self.ticks = t, buf, 0, (), 0

    def at(self, d):
        return lax.rem(self.t.z + d + 8, 8)

    def wait(self):
        for copy in self.pending:
            copy.wait_recv()
        self.pending = ()

    def late_hop(self):
        self.ticks += 1
        if self.ticks == LAST_HOP:
            self.hop()

    def hop(self):
        self.wait()
        t, d = self.t, self.hops
        self.hops += 1
        up, down = self.buf.at[self.at(-d)], self.buf.at[self.at(d)]
        if d == 3:
            n = self.buf.shape[1] // 2
            up = self.buf.at[self.at(-d), pl.ds(0, n)]
            down = self.buf.at[self.at(d), pl.ds(n, n)]
        self.pending = (t.send(up, up, t.dev_z(1)), t.send(down, down, t.dev_z(-1)))


def together(chains, tick=None, lead=0):
    chains = list(chains)
    ended = object()
    for _ in range(lead):
        next(chains[0])
    while chains:
        for one in list(chains):
            if next(one, ended) is ended:
                chains.remove(one)
        if tick is not None:
            tick()


def attend(t, mem, w, beside):
    u = t.user
    copies = []
    for dy, dx, dc in OTHERS:
        if dc == 0:
            y, x, c = t.shifted(dy, dx, dc)
            copies.append((dy, dx, t.send(mem.query.at[owned(y, x, c)[0]], mem.keys.at[t.me], (t.z, y, x, c))))
    mem.keys[t.me] = mem.query[u]
    twins = [t.send(mem.keys.at[t.me], mem.keys.at[t.me], t.partner())]
    beside()
    w.hop()
    for dy, dx, copy in reversed(copies):
        copy.wait_recv()
        y, x = lax.rem(t.y - dy + 4, 4), lax.rem(t.x - dx + 4, 4)
        ref = mem.keys.at[(y * 4 + x) * 2 + t.c]
        twins.append(t.send(ref, ref, t.partner()))
    for copy in mem.moved:
        copy.wait_recv()
    mem.own_behaviors.wait()
    for copy in twins:
        copy.wait_recv()
    behaviors = mem.behaviors[...].reshape(WIDTH, QUARTER)
    s = dot(mem.keys[...].reshape(WIDTH, CANDS), behaviors, ((0,), (0,)))
    s = s * (1.0 / math.sqrt(WIDTH))
    at = lax.broadcasted_iota(jnp.int32, s.shape, 1) + t.quarter * QUARTER
    live = at < mem.lengths[u]
    s = jnp.where(live, s, -1e30)
    highest = jnp.max(s, axis=1, keepdims=True)
    e = jnp.where(live, jnp.exp(s - highest), 0.0)
    total = jnp.sum(e, axis=1, keepdims=True)
    some = total > 0.0
    total = jnp.where(some, total, 1.0)
    level = jnp.where(some, highest + jnp.log(total), -1e30)
    level = jnp.broadcast_to(level, (CANDS, 128))
    mem.levels[...] = level
    mem.level_tx[...] = level.T[:8]
    mem.level_copies = [
        t.send(mem.level_tx, mem.level_rx.at[i], dev) for i, (dev, _) in enumerate(owners(t))
    ]
    p = (e / total).astype(BF)
    for i in range(4):
        mem.means[i] = dot(p, mem.behaviors[pl.ds(8 * i, 8)].reshape(FEATURES, QUARTER), ((1,), (1,)))


def owners(t):
    x = t.x + 1 - 2 * lax.rem(t.x, 2)
    result = []
    for xx, c in ((x, 1 - t.c), (x, t.c), (t.x, 1 - t.c)):
        result.append(((t.z, t.y, xx, c), owned(t.y, xx, c)[1]))
    return result


def chain(t, h, mem, w):
    rows = pl.ds(h * ROWS, ROWS)
    copies = []
    for i, (dev, quarter) in enumerate(owners(t)):
        mem.mean_tx[h, i] = mem.means[quarter, rows, :].astype(BF)
        copies.append(t.send(mem.mean_tx.at[h, i], mem.mean_rx.at[h, i], dev))
    yield
    if h == 0:
        for copy in mem.level_copies:
            copy.wait_recv()
        levels = [mem.levels[...]]
        levels += [jnp.broadcast_to(mem.level_rx[i][:1], (128, CANDS)).T for i in range(3)]
        top = jnp.maximum(jnp.maximum(levels[0], levels[1]), jnp.maximum(levels[2], levels[3]))
        shares = [jnp.exp(level - top) for level in levels]
        scale = 1.0 / (shares[0] + shares[1] + shares[2] + shares[3])
        for i in range(4):
            mem.shares[i] = shares[i] * scale

    def share(i):
        return jnp.concatenate([mem.shares[i, rows, :]] * (FEATURES // 128), axis=1)

    total = mem.means[t.quarter, rows, :] * share(0)
    for i in (2, 1, 0):
        copies[i].wait_recv()
        total += mem.mean_rx[h, i].astype(F32) * share(i + 1)
    mem.pooled[h, t.quarter, t.user] = total.astype(BF)

    def pooled_slot(a, b):
        user, quarter = owned(*t.chip(a, b), t.c)
        return mem.pooled.at[h, quarter, user]

    yield from all_gather(t, pooled_slot, MEAN_HALVES)
    if h == 0:
        w.wait()

    n = 256
    for i in range(TOKENS // n):
        acc = jnp.zeros((n, 2 * UNITS), F32)
        squares = jnp.zeros((n, 1), F32)
        for k in range(4):
            x = mem.pooled[h, k, pl.ds(4 * i, 4)].reshape(n, FEATURES)
            acc += dot(x, mem.weights[pl.ds(2 * k, 2), :, pl.ds(0, 2 * UNITS)].reshape(FEATURES, 2 * UNITS))
            v = x.astype(F32)
            squares += jnp.sum(v * v, axis=1, keepdims=True)
        acc = acc * lax.rsqrt(squares * (1.0 / WIDTH) + 1e-6)
        gate, upward = acc[:, :UNITS], acc[:, UNITS:]
        value = gate / (1.0 + jnp.exp(-gate)) * upward
        mem.hidden[h, :, pl.ds(i * n, n)] = value.T.astype(BF)
    yield

    def outputs(core, group):
        parts = []
        for i in range(4):
            y = group + core * (i - group)
            x = i + core * (group - i)
            m = (y * 4 + x) * 2 + core
            at = pl.multiple_of(lax.rem(m, 4) * FEATS, FEATS)
            parts.append(mem.weights[m // 4, pl.ds(at, FEATS), pl.ds(2 * UNITS, UNITS)])
        return dot(jnp.concatenate(parts, axis=0), mem.hidden[h])

    total = yield from reduce_scatter(
        t,
        outputs,
        *(ref.at[h] for ref in mem.out_1),
        *(ref.at[h] for ref in mem.out_2),
    )
    mem.result[h] = total


class Memory:
    pass


def kernel(
    cand_in,
    behaviors_in,
    lengths,
    bilinear_in,
    gain,
    w_gate_in,
    w_up_in,
    w_down_in,
    out,
    behaviors,
    bilinear,
    raw_weights,
    weights,
    cands,
    query,
    keys,
    means,
    mean_tx,
    mean_rx,
    levels,
    level_tx,
    level_rx,
    shares,
    pooled,
    hidden,
    result,
    *rest,
):
    send_sem, recv_sem, in_sem = rest[-3:]
    t = Torus(send_sem, recv_sem)
    mem = Memory()
    mem.behaviors, mem.bilinear, mem.weights, mem.cands = behaviors, bilinear, weights, cands
    mem.query, mem.keys, mem.pooled, mem.hidden = query, keys, pooled, hidden
    mem.means, mem.mean_tx, mem.mean_rx, mem.shares = means, mean_tx, mean_rx, shares
    mem.levels, mem.level_tx, mem.level_rx = levels, level_tx, level_rx
    mem.lengths, mem.result = lengths, result
    mem.out_1, mem.out_2 = rest[0:5], rest[5:8]

    started = []

    def fetch(src, dst):
        copy = pltpu.make_async_copy(src, dst, in_sem.at[len(started)])
        copy.start()
        started.append(copy)
        return copy

    cand_copies = [
        fetch(
            cand_in.at[u],
            cands.at[u // CHUNK_USERS, t.me, :, pl.ds(u % CHUNK_USERS * CANDS, CANDS)],
        )
        for u in range(USERS_HERE)
    ]
    weight_copies = [
        fetch(w, raw_weights.at[i]) for i, w in enumerate((w_gate_in, w_up_in, w_down_in))
    ]
    bilinear_copy = fetch(bilinear_in, bilinear)

    def behaviors_of(y, x, core):
        user, quarter = owned(y, x, core)
        at = pl.multiple_of(quarter * QUARTER, QUARTER)
        return behaviors_in.at[user, :, pl.ds(at, QUARTER)]

    mem.own_behaviors = fetch(behaviors_of(t.y, t.x, t.c), behaviors.at[t.me])
    t.barrier()

    to_move = list(OTHERS)
    mem.moved = []

    def move_behaviors(count):
        for _ in range(min(count, len(to_move))):
            y, x, c = t.shifted(*to_move.pop(0))
            mem.moved.append(t.send(behaviors_of(y, x, c), behaviors.at[t.me], (t.z, y, x, c)))

    def cand_slot(h):
        def slot(a, b):
            y, x = t.chip(a, b)
            return cands.at[h, (y * 4 + x) * 2 + t.c]

        return slot

    w = Weights(t, weights)
    for copy in cand_copies:
        copy.wait()
    gathers = [all_gather(t, cand_slot(h), CAND_HALVES) for h in range(CHUNKS)]
    for one in gathers:
        next(one)

    own_gain = gain[pl.ds(pl.multiple_of(t.z * UNITS, UNITS), UNITS)].reshape(1, UNITS)
    own_gain = jnp.broadcast_to(own_gain, (128, UNITS)).T
    own_gain = jnp.concatenate([own_gain, own_gain], axis=1)
    for i in range(3):
        weight_copies[i].wait()
        v = raw_weights[i].astype(F32)
        v = v * own_gain if i < 2 else v.T
        weights[t.z, :, pl.ds(i * UNITS, UNITS)] = v.astype(BF)
    w.hop()

    steps = iter(range(1, 99))

    def beside():
        step = next(steps)
        if step == MOVE_AT:
            move_behaviors(MOVE)
        if step == SECOND_HOP:
            w.hop()

    together(gathers, beside)
    bilinear_copy.wait()
    for h in range(CHUNKS):
        q = dot(bilinear[...], cands[h].reshape(WIDTH, TOKENS)).astype(BF)
        for u in range(CHUNK_USERS):
            query[h * CHUNK_USERS + u] = q[:, u * CANDS : (u + 1) * CANDS]
    attend(t, mem, w, lambda: move_behaviors(len(to_move)))
    together([chain(t, h, mem, w) for h in range(CHUNKS)], w.late_hop, LEAD)
    for u in range(USERS_HERE):
        parts = [result[h, :, pl.ds(u // 2 * 128, 128)] for h in range(CHUNKS)]
        if u % 2 == 0:
            both = jnp.concatenate([part[:, :ROWS] for part in parts], axis=1)
        else:
            both = jnp.concatenate([part[:, ROWS:] for part in parts], axis=1)
        out[u] = both.astype(BF)
    t.finish()


def exchange_buffers(rows, piece, width):
    return (
        pltpu.VMEM((CHUNKS, 4, rows, width), BF),
        pltpu.VMEM((CHUNKS, 4, rows, width), BF),
        pltpu.VMEM((CHUNKS, 4, rows, width), F32),
        pltpu.VMEM((CHUNKS, 3, rows, width), BF),
        pltpu.VMEM((CHUNKS, 3, rows, width), BF),
        pltpu.VMEM((CHUNKS, 4, piece, width), F32),
        pltpu.VMEM((CHUNKS, 3, piece, width), BF),
        pltpu.VMEM((CHUNKS, 3, piece, width), BF),
    )


def shards(behaviors, candidates, lengths, bilinear, norm_gain, w_gate, w_up, w_down):
    vmem = pl.BlockSpec(memory_space=pltpu.VMEM)
    hbm = pl.BlockSpec(memory_space=pl.ANY)
    smem = pl.BlockSpec(memory_space=pltpu.SMEM)
    return pl.pallas_call(
        kernel,
        out_shape=jax.ShapeDtypeStruct(candidates.shape, BF),
        in_specs=[hbm, hbm, smem, hbm, vmem, hbm, hbm, hbm],
        out_specs=vmem,
        scratch_shapes=[
            pltpu.VMEM((32, FEATS, QUARTER), BF),
            pltpu.VMEM(bilinear.shape, BF),
            pltpu.VMEM((3, UNITS, UNITS), BF),
            pltpu.VMEM((8, UNITS, 3 * UNITS), BF),
            pltpu.VMEM((CHUNKS, 32, FEATS, TOKENS), BF),
            pltpu.VMEM((USERS_HERE, FEATS, CANDS), BF),
            pltpu.VMEM((32, FEATS, CANDS), BF),
            pltpu.VMEM((4, CANDS, FEATURES), F32),
            pltpu.VMEM((CHUNKS, 3, ROWS, FEATURES), BF),
            pltpu.VMEM((CHUNKS, 3, ROWS, FEATURES), BF),
            pltpu.VMEM((CANDS, 128), F32),
            pltpu.VMEM((8, CANDS), F32),
            pltpu.VMEM((3, 8, CANDS), F32),
            pltpu.VMEM((4, CANDS, 128), F32),
            pltpu.VMEM((CHUNKS, 4, USERS_HERE, ROWS, FEATURES), BF),
            pltpu.VMEM((CHUNKS, UNITS, TOKENS), BF),
            pltpu.VMEM((CHUNKS, FEATS, TOKENS), F32),
            *exchange_buffers(256, FEATS, TOKENS),
            pltpu.SemaphoreType.DMA((N_SEMS,)),
            pltpu.SemaphoreType.DMA((N_SEMS,)),
            pltpu.SemaphoreType.DMA((16,)),
        ],
        compiler_params=pltpu.CompilerParams(
            collective_id=0, has_side_effects=True, vmem_limit_bytes=56 * 1024 * 1024
        ),
    )(
        candidates,
        behaviors,
        lengths,
        bilinear,
        norm_gain,
        w_gate,
        w_up,
        w_down,
    )


def solution(mesh):
    finer = Mesh(mesh.devices.reshape(mesh.shape["dp"], 4, 4, 2), ("dp", "mp_0", "mp_1", "mp_2"))
    return jax.shard_map(
        shards,
        mesh=finer,
        in_specs=(
            P("dp", MP, None),
            P("dp", MP, None),
            P("dp"),
            P(MP, None),
            P(),
            P("dp", MP),
            P("dp", MP),
            P(MP, "dp"),
        ),
        out_specs=P("dp", MP, None),
        check_vma=False,
    )
```

```python
import math

import jax
import jax.numpy as jnp
from jax import lax
from jax.experimental import pallas as pl
from jax.experimental.pallas import tpu as pltpu
from jax.sharding import Mesh
from jax.sharding import PartitionSpec as P

MP = ("mp_0", "mp_1", "mp_2")
MESH = pl.DeviceIdType.MESH
BF = jnp.bfloat16
F32 = jnp.float32
USERS_HERE = 8
CANDS = 128
WIDTH = 2048
BEHAVIORS = 1024
CHUNKS = 2
CHUNK_USERS = USERS_HERE // CHUNKS
TOKENS = CHUNK_USERS * CANDS
QUARTER = BEHAVIORS // 4
FEATURES = WIDTH // 4
ROWS = CANDS // CHUNKS
OTHERS = sorted(
    ((dy, dx, dc) for dy in range(4) for dx in range(4) for dc in range(2) if dy + dx + dc),
    key=lambda d: (-min(d[0], 4 - d[0]) - min(d[1], 4 - d[1]), d),
)
LEAD = 0
SECOND_HOP = 8
LAST_HOP = 6
MOVES = (0, 0, 0, 20)
CAND_HALVES = 32
MEAN_HALVES = None
FEATS = 64
UNITS = 256
N_OUT, N_INTO = 43, 126


class Torus:
    def __init__(self, send_sem, recv_sem):
        self.z = lax.axis_index("dp")
        self.y = lax.axis_index("mp_0")
        self.x = lax.axis_index("mp_1")
        self.c = lax.axis_index("mp_2")
        self.a = self.x + self.c * (self.y - self.x)
        self.b = self.y + self.c * (self.x - self.y)
        self.me = (self.y * 4 + self.x) * 2 + self.c
        self.user, self.quarter = owned(self.y, self.x, self.c)
        self.send_sem, self.recv_sem = send_sem, recv_sem
        self.copies, self.ends = [], []
        self.outs = self.intos = 0

    def chip(self, a, b):
        return b + self.c * (a - b), a + self.c * (b - a)

    def shifted(self, dy, dx, dc):
        core = 1 - self.c if dc else self.c
        return lax.rem(self.y + dy, 4), lax.rem(self.x + dx, 4), core

    def dev_a(self, d):
        c = self.c
        return (self.z, lax.rem(self.y + c * d + 4, 4), lax.rem(self.x + (1 - c) * d + 4, 4), c)

    def dev_b(self, d):
        c = self.c
        return (self.z, lax.rem(self.y + (1 - c) * d + 4, 4), lax.rem(self.x + c * d + 4, 4), c)

    def dev_z(self, d):
        return (lax.rem(self.z + d + 8, 8), self.y, self.x, self.c)

    def partner(self):
        return (self.z, self.y, self.x, 1 - self.c)

    def new_out(self):
        self.outs += 1
        return self.outs - 1

    def new_into(self):
        self.intos += 1
        return self.intos - 1

    def copy(self, src, dst, dev, out, into):
        return pltpu.make_async_remote_copy(
            src_ref=src,
            dst_ref=dst,
            send_sem=self.send_sem.at[out],
            recv_sem=self.recv_sem.at[into],
            device_id=dev,
            device_id_type=MESH,
        )

    def send(self, src, dst, dev, out=None, into=None):
        alone = out is None
        out = self.new_out() if alone else out
        copy = self.copy(src, dst, dev, out, self.new_into() if into is None else into)
        copy.start()
        if alone:
            self.copies.append(copy)
        return copy

    def await_all(self, ref, into):
        self.copy(ref, ref, self.partner(), 0, into).wait_recv()

    def await_sent(self, ref, out):
        self.ends.append(self.copy(ref, ref, self.partner(), out, 0))

    def finish(self):
        for copy in self.copies + self.ends:
            copy.wait_send()

    def barrier(self):
        sem = pltpu.get_barrier_semaphore()
        peers = [self.dev_z(1), self.dev_z(-1)]
        peers += [(self.z, *self.shifted(*d)) for d in OTHERS]
        for dev in peers:
            pl.semaphore_signal(sem, inc=1, device_id=dev, device_id_type=MESH)
        pl.semaphore_wait(sem, len(peers))


def owned(y, x, core):
    return y * 2 + x // 2, lax.rem(x, 2) * 2 + core


def all_gather(t, slot, blocks, halves=None):
    out, into = t.new_out(), t.new_into()

    def block(da, db):
        return slot(lax.rem(t.a + da + 4, 4), lax.rem(t.b + db + 4, 4))

    def whole(da, db, dev):
        ref = block(da, db)
        return t.send(ref, ref, dev, out)

    def double(da, db):
        ref = block(da, db)
        t.send(ref, ref, t.partner(), out, into)

    def part(da, db, h, dev):
        ref = block(da, db).at[pl.ds(h * halves, halves), :]
        return t.send(ref, ref, dev, out)

    far = (2, 1, -1) if halves is None else (1, -1)
    row = {d: whole(0, 0, t.dev_a(d)) for d in (2, 1, -1)}
    column = {(0, d): whole(0, 0, t.dev_b(d)) for d in far}
    double(0, 0)
    for q in (-1, 1, 2):
        yield
        row[q].wait_recv()
        for d in far:
            column[-q, d] = whole(-q, 0, t.dev_b(d))
        double(-q, 0)
    ends = {}
    for (q, d), copy in column.items():
        yield
        copy.wait_recv()
        if halves is not None:
            ends.setdefault(q, []).append(part(q, -d, 0 if d == 1 else 1, t.dev_b(d)))
        double(q, -d)
    for q, copies in ends.items():
        yield
        for copy in copies:
            copy.wait_recv()
        double(q, 2)
    yield
    t.await_all(blocks(16), into)
    t.await_sent(blocks(31), out)


def ring_sum(t, p, dev, terms, tx, rx):
    copies = []
    for i, d in enumerate((2, 1, -1)):
        tx[i] = terms[lax.rem(p + d + 4, 4)].astype(tx.dtype)
        copies.append(t.send(tx.at[i], rx.at[i], dev(d)))
    total = terms[p]
    for i in (1, 2, 0):
        yield
        copies[i].wait_recv()
        total += rx[i].astype(F32)
    return total


def reduce_scatter(t, term, twin_tx, twin_rx, terms, tx, rx, terms_2, tx_2, rx_2):
    other = 1 - t.c
    twins = []
    for d in (2, 1, -1, 0):
        g = lax.rem(t.a + d + 4, 4)
        twin_tx[g] = term(other, g).astype(twin_tx.dtype)
        twins.append(t.send(twin_tx.at[g], twin_rx.at[g], t.partner()))
    order = [lax.rem(t.b + d + 4, 4) for d in (2, 1, -1, 0)]
    for g in order:
        terms[g] = term(t.c, g)
    yield
    for copy, g in zip(twins, order):
        copy.wait_recv()
        terms[g] += twin_rx[g].astype(F32)
    total = yield from ring_sum(t, t.b, t.dev_b, terms, tx, rx)
    n = terms_2.shape[1]
    for i in range(4):
        terms_2[i] = total[i * n : (i + 1) * n]
    return (yield from ring_sum(t, t.a, t.dev_a, terms_2, tx_2, rx_2))


def dot(a, b, dims=((1,), (0,))):
    return lax.dot_general(a, b, (dims, ((), ())), preferred_element_type=F32)


class Weights:
    def __init__(self, t, buf):
        self.t, self.buf, self.hops, self.pending, self.ticks = t, buf, 0, (), 0

    def at(self, d):
        return lax.rem(self.t.z + d + 8, 8)

    def wait(self):
        for copy in self.pending:
            copy.wait_recv()
        self.pending = ()

    def late_hop(self):
        self.ticks += 1
        if self.ticks == LAST_HOP:
            self.hop()

    def hop(self):
        self.wait()
        t, d = self.t, self.hops
        self.hops += 1
        up, down = self.buf.at[self.at(-d)], self.buf.at[self.at(d)]
        if d == 3:
            n = self.buf.shape[1] // 2
            up = self.buf.at[self.at(-d), pl.ds(0, n)]
            down = self.buf.at[self.at(d), pl.ds(n, n)]
        self.pending = (t.send(up, up, t.dev_z(1)), t.send(down, down, t.dev_z(-1)))


def together(chains, tick=None, lead=0):
    chains = list(chains)
    ended = object()
    for _ in range(lead):
        next(chains[0])
    while chains:
        for one in list(chains):
            if next(one, ended) is ended:
                chains.remove(one)
        if tick is not None:
            tick()


def attend(t, mem, w, beside):
    u = t.user
    copies = []
    out, into = t.new_out(), t.new_into()

    def double(ref):
        t.send(ref, ref, t.partner(), out, into)

    for dy, dx, dc in OTHERS:
        if dc == 0:
            y, x, c = t.shifted(dy, dx, dc)
            copies.append((dy, dx, t.send(mem.query.at[owned(y, x, c)[0]], mem.keys.at[t.me], (t.z, y, x, c), out)))
    mem.keys[t.me] = mem.query[u]
    double(mem.keys.at[t.me])
    beside()
    w.hop()
    for dy, dx, copy in reversed(copies):
        copy.wait_recv()
        y, x = lax.rem(t.y - dy + 4, 4), lax.rem(t.x - dx + 4, 4)
        double(mem.keys.at[(y * 4 + x) * 2 + t.c])
    t.await_all(mem.behaviors.at[pl.ds(0, 31)], mem.move_into)
    t.await_sent(mem.behaviors.at[pl.ds(0, 31)], mem.move_out)
    mem.own_behaviors.wait()
    t.await_all(mem.keys.at[pl.ds(0, 16)], into)
    t.await_sent(mem.keys.at[pl.ds(0, 31)], out)
    behaviors = mem.behaviors[...].reshape(WIDTH, QUARTER)
    s = dot(mem.keys[...].reshape(WIDTH, CANDS), behaviors, ((0,), (0,)))
    s = s * (1.0 / math.sqrt(WIDTH))
    at = lax.broadcasted_iota(jnp.int32, s.shape, 1) + t.quarter * QUARTER
    live = at < mem.lengths[u]
    s = jnp.where(live, s, -1e30)
    highest = jnp.max(s, axis=1, keepdims=True)
    e = jnp.where(live, jnp.exp(s - highest), 0.0)
    total = jnp.sum(e, axis=1, keepdims=True)
    some = total > 0.0
    total = jnp.where(some, total, 1.0)
    level = jnp.where(some, highest + jnp.log(total), -1e30)
    level = jnp.broadcast_to(level, (CANDS, 128))
    mem.levels[...] = level
    mem.level_tx[...] = level.T[:8]
    mem.level_copies = [
        t.send(mem.level_tx, mem.level_rx.at[i], dev) for i, (dev, _) in enumerate(owners(t))
    ]
    p = (e / total).astype(BF)
    for i in range(4):
        mem.means[i] = dot(p, mem.behaviors[pl.ds(8 * i, 8)].reshape(FEATURES, QUARTER), ((1,), (1,)))


def owners(t):
    x = t.x + 1 - 2 * lax.rem(t.x, 2)
    result = []
    for xx, c in ((x, 1 - t.c), (x, t.c), (t.x, 1 - t.c)):
        result.append(((t.z, t.y, xx, c), owned(t.y, xx, c)[1]))
    return result


def chain(t, h, mem, w):
    rows = pl.ds(h * ROWS, ROWS)
    copies = []
    for i, (dev, quarter) in enumerate(owners(t)):
        mem.mean_tx[h, i] = mem.means[quarter, rows, :].astype(BF)
        copies.append(t.send(mem.mean_tx.at[h, i], mem.mean_rx.at[h, i], dev))
    yield
    if h == 0:
        for copy in mem.level_copies:
            copy.wait_recv()
        levels = [mem.levels[...]]
        levels += [jnp.broadcast_to(mem.level_rx[i][:1], (128, CANDS)).T for i in range(3)]
        top = jnp.maximum(jnp.maximum(levels[0], levels[1]), jnp.maximum(levels[2], levels[3]))
        shares = [jnp.exp(level - top) for level in levels]
        scale = 1.0 / (shares[0] + shares[1] + shares[2] + shares[3])
        for i in range(4):
            mem.shares[i] = shares[i] * scale

    def share(i):
        return jnp.concatenate([mem.shares[i, rows, :]] * (FEATURES // 128), axis=1)

    total = mem.means[t.quarter, rows, :] * share(0)
    for i in (2, 1, 0):
        copies[i].wait_recv()
        total += mem.mean_rx[h, i].astype(F32) * share(i + 1)
    mem.pooled[h, t.quarter * USERS_HERE + t.user] = total.astype(BF)

    def pooled_slot(a, b):
        user, quarter = owned(*t.chip(a, b), t.c)
        return mem.pooled.at[h, quarter * USERS_HERE + user]

    yield from all_gather(
        t, pooled_slot, lambda n: mem.pooled.at[h, pl.ds(0, n)], MEAN_HALVES
    )
    if h == 0:
        w.wait()

    n = 256
    for i in range(TOKENS // n):
        acc = jnp.zeros((n, 2 * UNITS), F32)
        squares = jnp.zeros((n, 1), F32)
        for k in range(4):
            x = mem.pooled[h, pl.ds(USERS_HERE * k + 4 * i, 4)].reshape(n, FEATURES)
            acc += dot(x, mem.weights[pl.ds(2 * k, 2), :, pl.ds(0, 2 * UNITS)].reshape(FEATURES, 2 * UNITS))
            v = x.astype(F32)
            squares += jnp.sum(v * v, axis=1, keepdims=True)
        acc = acc * lax.rsqrt(squares * (1.0 / WIDTH) + 1e-6)
        gate, upward = acc[:, :UNITS], acc[:, UNITS:]
        value = gate / (1.0 + jnp.exp(-gate)) * upward
        mem.hidden[h, :, pl.ds(i * n, n)] = value.T.astype(BF)
    yield

    def outputs(core, group):
        parts = []
        for i in range(4):
            y = group + core * (i - group)
            x = i + core * (group - i)
            m = (y * 4 + x) * 2 + core
            at = pl.multiple_of(lax.rem(m, 4) * FEATS, FEATS)
            parts.append(mem.weights[m // 4, pl.ds(at, FEATS), pl.ds(2 * UNITS, UNITS)])
        return dot(jnp.concatenate(parts, axis=0), mem.hidden[h])

    total = yield from reduce_scatter(
        t,
        outputs,
        *(ref.at[h] for ref in mem.out_1),
        *(ref.at[h] for ref in mem.out_2),
    )
    mem.result[h] = total


class Memory:
    pass


def kernel(
    cand_in,
    behaviors_in,
    lengths,
    bilinear_in,
    gain,
    w_gate_in,
    w_up_in,
    w_down_in,
    out,
    behaviors,
    bilinear,
    raw_weights,
    weights,
    cands,
    query,
    keys,
    means,
    mean_tx,
    mean_rx,
    levels,
    level_tx,
    level_rx,
    shares,
    pooled,
    hidden,
    result,
    *rest,
):
    send_sem, recv_sem, in_sem = rest[-3:]
    t = Torus(send_sem, recv_sem)
    mem = Memory()
    mem.behaviors, mem.bilinear, mem.weights, mem.cands = behaviors, bilinear, weights, cands
    mem.query, mem.keys, mem.pooled, mem.hidden = query, keys, pooled, hidden
    mem.means, mem.mean_tx, mem.mean_rx, mem.shares = means, mean_tx, mean_rx, shares
    mem.levels, mem.level_tx, mem.level_rx = levels, level_tx, level_rx
    mem.lengths, mem.result = lengths, result
    mem.out_1, mem.out_2 = rest[0:5], rest[5:8]

    started = []

    def fetch(src, dst):
        copy = pltpu.make_async_copy(src, dst, in_sem.at[len(started)])
        copy.start()
        started.append(copy)
        return copy

    cand_copies = [
        fetch(
            cand_in.at[u],
            cands.at[u // CHUNK_USERS, t.me, :, pl.ds(u % CHUNK_USERS * CANDS, CANDS)],
        )
        for u in range(USERS_HERE)
    ]
    weight_copies = [
        fetch(w, raw_weights.at[i]) for i, w in enumerate((w_gate_in, w_up_in, w_down_in))
    ]
    bilinear_copy = fetch(bilinear_in, bilinear)

    def behaviors_of(y, x, core):
        user, quarter = owned(y, x, core)
        at = pl.multiple_of(quarter * QUARTER, QUARTER)
        return behaviors_in.at[user, :, pl.ds(at, QUARTER)]

    mem.own_behaviors = fetch(behaviors_of(t.y, t.x, t.c), behaviors.at[t.me])
    t.barrier()

    to_move = list(OTHERS)
    mem.move_out, mem.move_into = t.new_out(), t.new_into()

    def move_behaviors(count):
        for _ in range(min(count, len(to_move))):
            y, x, c = t.shifted(*to_move.pop(0))
            src, dst = behaviors_of(y, x, c), behaviors.at[t.me]
            t.send(src, dst, (t.z, y, x, c), mem.move_out, mem.move_into)

    def cand_slot(h):
        def slot(a, b):
            y, x = t.chip(a, b)
            return cands.at[h, (y * 4 + x) * 2 + t.c]

        return slot

    w = Weights(t, weights)
    for copy in cand_copies:
        copy.wait()
    gathers = [
        all_gather(t, cand_slot(h), lambda n, h=h: cands.at[h, pl.ds(0, n)], CAND_HALVES)
        for h in range(CHUNKS)
    ]
    for one in gathers:
        next(one)

    own_gain = gain[pl.ds(pl.multiple_of(t.z * UNITS, UNITS), UNITS)].reshape(1, UNITS)
    own_gain = jnp.broadcast_to(own_gain, (128, UNITS)).T
    own_gain = jnp.concatenate([own_gain, own_gain], axis=1)
    for i in range(3):
        weight_copies[i].wait()
        v = raw_weights[i].astype(F32)
        v = v * own_gain if i < 2 else v.T
        weights[t.z, :, pl.ds(i * UNITS, UNITS)] = v.astype(BF)
    w.hop()

    steps = iter(range(1, 99))

    def beside():
        step = next(steps)
        if step < len(MOVES):
            move_behaviors(MOVES[step])
        if step == SECOND_HOP:
            w.hop()

    move_behaviors(MOVES[0])
    together(gathers, beside)
    bilinear_copy.wait()
    for h in range(CHUNKS):
        q = dot(bilinear[...], cands[h].reshape(WIDTH, TOKENS)).astype(BF)
        for u in range(CHUNK_USERS):
            query[h * CHUNK_USERS + u] = q[:, u * CANDS : (u + 1) * CANDS]
    attend(t, mem, w, lambda: move_behaviors(len(to_move)))
    together([chain(t, h, mem, w) for h in range(CHUNKS)], w.late_hop, LEAD)
    for u in range(USERS_HERE):
        parts = [result[h, :, pl.ds(u // 2 * 128, 128)] for h in range(CHUNKS)]
        if u % 2 == 0:
            both = jnp.concatenate([part[:, :ROWS] for part in parts], axis=1)
        else:
            both = jnp.concatenate([part[:, ROWS:] for part in parts], axis=1)
        out[u] = both.astype(BF)
    t.finish()
    assert (t.outs, t.intos) == (N_OUT, N_INTO), (t.outs, t.intos)


def exchange_buffers(rows, piece, width):
    return (
        pltpu.VMEM((CHUNKS, 4, rows, width), BF),
        pltpu.VMEM((CHUNKS, 4, rows, width), BF),
        pltpu.VMEM((CHUNKS, 4, rows, width), F32),
        pltpu.VMEM((CHUNKS, 3, rows, width), BF),
        pltpu.VMEM((CHUNKS, 3, rows, width), BF),
        pltpu.VMEM((CHUNKS, 4, piece, width), F32),
        pltpu.VMEM((CHUNKS, 3, piece, width), BF),
        pltpu.VMEM((CHUNKS, 3, piece, width), BF),
    )


def shards(behaviors, candidates, lengths, bilinear, norm_gain, w_gate, w_up, w_down):
    vmem = pl.BlockSpec(memory_space=pltpu.VMEM)
    hbm = pl.BlockSpec(memory_space=pl.ANY)
    smem = pl.BlockSpec(memory_space=pltpu.SMEM)
    return pl.pallas_call(
        kernel,
        out_shape=jax.ShapeDtypeStruct(candidates.shape, BF),
        in_specs=[hbm, hbm, smem, hbm, vmem, hbm, hbm, hbm],
        out_specs=vmem,
        scratch_shapes=[
            pltpu.VMEM((32, FEATS, QUARTER), BF),
            pltpu.VMEM(bilinear.shape, BF),
            pltpu.VMEM((3, UNITS, UNITS), BF),
            pltpu.VMEM((8, UNITS, 3 * UNITS), BF),
            pltpu.VMEM((CHUNKS, 32, FEATS, TOKENS), BF),
            pltpu.VMEM((USERS_HERE, FEATS, CANDS), BF),
            pltpu.VMEM((32, FEATS, CANDS), BF),
            pltpu.VMEM((4, CANDS, FEATURES), F32),
            pltpu.VMEM((CHUNKS, 3, ROWS, FEATURES), BF),
            pltpu.VMEM((CHUNKS, 3, ROWS, FEATURES), BF),
            pltpu.VMEM((CANDS, 128), F32),
            pltpu.VMEM((8, CANDS), F32),
            pltpu.VMEM((3, 8, CANDS), F32),
            pltpu.VMEM((4, CANDS, 128), F32),
            pltpu.VMEM((CHUNKS, 4 * USERS_HERE, ROWS, FEATURES), BF),
            pltpu.VMEM((CHUNKS, UNITS, TOKENS), BF),
            pltpu.VMEM((CHUNKS, FEATS, TOKENS), F32),
            *exchange_buffers(256, FEATS, TOKENS),
            pltpu.SemaphoreType.DMA((N_OUT,)),
            pltpu.SemaphoreType.DMA((N_INTO,)),
            pltpu.SemaphoreType.DMA((16,)),
        ],
        compiler_params=pltpu.CompilerParams(
            collective_id=0, has_side_effects=True, vmem_limit_bytes=56 * 1024 * 1024
        ),
    )(
        candidates,
        behaviors,
        lengths,
        bilinear,
        norm_gain,
        w_gate,
        w_up,
        w_down,
    )


def solution(mesh):
    finer = Mesh(mesh.devices.reshape(mesh.shape["dp"], 4, 4, 2), ("dp", "mp_0", "mp_1", "mp_2"))
    return jax.shard_map(
        shards,
        mesh=finer,
        in_specs=(
            P("dp", MP, None),
            P("dp", MP, None),
            P("dp"),
            P(MP, None),
            P(),
            P("dp", MP),
            P("dp", MP),
            P(MP, "dp"),
        ),
        out_specs=P("dp", MP, None),
        check_vma=False,
    )
```

```python
import math

import jax
import jax.numpy as jnp
from jax import lax
from jax.experimental import pallas as pl
from jax.experimental.pallas import tpu as pltpu
from jax.sharding import Mesh
from jax.sharding import PartitionSpec as P

MP = ("mp_0", "mp_1", "mp_2")
MESH = pl.DeviceIdType.MESH
BF = jnp.bfloat16
F32 = jnp.float32
USERS_HERE = 8
CANDS = 128
WIDTH = 2048
BEHAVIORS = 1024
CHUNKS = 2
CHUNK_USERS = USERS_HERE // CHUNKS
TOKENS = CHUNK_USERS * CANDS
QUARTER = BEHAVIORS // 4
FEATURES = WIDTH // 4
ROWS = CANDS // CHUNKS
OTHERS = sorted(
    ((dy, dx, dc) for dy in range(4) for dx in range(4) for dc in range(2) if dy + dx + dc),
    key=lambda d: (-min(d[0], 4 - d[0]) - min(d[1], 4 - d[1]), d),
)
LEAD = 0
SECOND_HOP = 8
LAST_HOP = 4
MOVES = (4, 0, 0, 5, 5, 5, 5, 5, 5)
CAND_HALVES = 32
MEAN_HALVES = 32
FEATS = 64
UNITS = 256
N_OUT, N_INTO = 43, 134


class Torus:
    def __init__(self, send_sem, recv_sem):
        self.z = lax.axis_index("dp")
        self.y = lax.axis_index("mp_0")
        self.x = lax.axis_index("mp_1")
        self.c = lax.axis_index("mp_2")
        self.a = self.x + self.c * (self.y - self.x)
        self.b = self.y + self.c * (self.x - self.y)
        self.me = (self.y * 4 + self.x) * 2 + self.c
        self.user, self.quarter = owned(self.y, self.x, self.c)
        self.send_sem, self.recv_sem = send_sem, recv_sem
        self.copies, self.ends = [], []
        self.outs = self.intos = 0

    def chip(self, a, b):
        return b + self.c * (a - b), a + self.c * (b - a)

    def shifted(self, dy, dx, dc):
        core = 1 - self.c if dc else self.c
        return lax.rem(self.y + dy, 4), lax.rem(self.x + dx, 4), core

    def dev_a(self, d):
        c = self.c
        return (self.z, lax.rem(self.y + c * d + 4, 4), lax.rem(self.x + (1 - c) * d + 4, 4), c)

    def dev_b(self, d):
        c = self.c
        return (self.z, lax.rem(self.y + (1 - c) * d + 4, 4), lax.rem(self.x + c * d + 4, 4), c)

    def dev_z(self, d):
        return (lax.rem(self.z + d + 8, 8), self.y, self.x, self.c)

    def partner(self):
        return (self.z, self.y, self.x, 1 - self.c)

    def new_out(self):
        self.outs += 1
        return self.outs - 1

    def new_into(self):
        self.intos += 1
        return self.intos - 1

    def copy(self, src, dst, dev, out, into):
        return pltpu.make_async_remote_copy(
            src_ref=src,
            dst_ref=dst,
            send_sem=self.send_sem.at[out],
            recv_sem=self.recv_sem.at[into],
            device_id=dev,
            device_id_type=MESH,
        )

    def send(self, src, dst, dev, out=None, into=None):
        alone = out is None
        out = self.new_out() if alone else out
        copy = self.copy(src, dst, dev, out, self.new_into() if into is None else into)
        copy.start()
        if alone:
            self.copies.append(copy)
        return copy

    def await_all(self, ref, into):
        self.copy(ref, ref, self.partner(), 0, into).wait_recv()

    def await_sent(self, ref, out):
        self.ends.append(self.copy(ref, ref, self.partner(), out, 0))

    def finish(self):
        for copy in self.copies + self.ends:
            copy.wait_send()

    def barrier(self):
        sem = pltpu.get_barrier_semaphore()
        peers = [self.dev_z(1), self.dev_z(-1)]
        peers += [(self.z, *self.shifted(*d)) for d in OTHERS]
        for dev in peers:
            pl.semaphore_signal(sem, inc=1, device_id=dev, device_id_type=MESH)
        pl.semaphore_wait(sem, len(peers))


def owned(y, x, core):
    return y * 2 + x // 2, lax.rem(x, 2) * 2 + core


def all_gather(t, slot, blocks, halves=None):
    out, into = t.new_out(), t.new_into()

    def block(da, db):
        return slot(lax.rem(t.a + da + 4, 4), lax.rem(t.b + db + 4, 4))

    def whole(da, db, dev):
        ref = block(da, db)
        return t.send(ref, ref, dev, out)

    def double(da, db):
        ref = block(da, db)
        t.send(ref, ref, t.partner(), out, into)

    def part(da, db, h, dev):
        ref = block(da, db).at[pl.ds(h * halves, halves), :]
        return t.send(ref, ref, dev, out)

    far = (2, 1, -1) if halves is None else (1, -1)
    row = {d: whole(0, 0, t.dev_a(d)) for d in (1, -1, 2)}
    column = {(0, d): whole(0, 0, t.dev_b(d)) for d in far}
    double(0, 0)
    for q in (-1, 1, 2):
        yield
        row[q].wait_recv()
        for d in far:
            column[-q, d] = whole(-q, 0, t.dev_b(d))
        double(-q, 0)
    ends = {}
    for (q, d), copy in column.items():
        yield
        copy.wait_recv()
        if halves is not None:
            ends.setdefault(q, []).append(part(q, -d, 0 if d == 1 else 1, t.dev_b(d)))
        double(q, -d)
    for q, copies in ends.items():
        yield
        for copy in copies:
            copy.wait_recv()
        double(q, 2)
    yield
    t.await_all(blocks(16), into)
    t.await_sent(blocks(31), out)


def ring_sum(t, p, dev, terms, tx, rx):
    copies = []
    for i, d in enumerate((2, 1, -1)):
        tx[i] = terms[lax.rem(p + d + 4, 4)].astype(tx.dtype)
        copies.append(t.send(tx.at[i], rx.at[i], dev(d)))
    total = terms[p]
    for i in (1, 2, 0):
        yield
        copies[i].wait_recv()
        total += rx[i].astype(F32)
    return total


def reduce_scatter(t, term, twin_tx, twin_rx, terms, tx, rx, terms_2, tx_2, rx_2):
    other = 1 - t.c
    twins = []
    for d in (2, 1, -1, 0):
        g = lax.rem(t.a + d + 4, 4)
        twin_tx[g] = term(other, g).astype(twin_tx.dtype)
        twins.append(t.send(twin_tx.at[g], twin_rx.at[g], t.partner()))
    order = [lax.rem(t.b + d + 4, 4) for d in (2, 1, -1, 0)]
    for g in order:
        terms[g] = term(t.c, g)
    yield
    for copy, g in zip(twins, order):
        copy.wait_recv()
        terms[g] += twin_rx[g].astype(F32)
    total = yield from ring_sum(t, t.b, t.dev_b, terms, tx, rx)
    n = terms_2.shape[1]
    for i in range(4):
        terms_2[i] = total[i * n : (i + 1) * n]
    return (yield from ring_sum(t, t.a, t.dev_a, terms_2, tx_2, rx_2))


def dot(a, b, dims=((1,), (0,))):
    return lax.dot_general(a, b, (dims, ((), ())), preferred_element_type=F32)


class Weights:
    def __init__(self, t, buf):
        self.t, self.buf, self.hops, self.pending, self.ticks = t, buf, 0, (), 0

    def at(self, d):
        return lax.rem(self.t.z + d + 8, 8)

    def wait(self):
        for copy in self.pending:
            copy.wait_recv()
        self.pending = ()

    def late_hop(self):
        self.ticks += 1
        if self.ticks == LAST_HOP:
            self.hop()

    def hop(self):
        self.wait()
        t, d = self.t, self.hops
        self.hops += 1
        up, down = self.buf.at[self.at(-d)], self.buf.at[self.at(d)]
        if d == 3:
            n = self.buf.shape[1] // 2
            up = self.buf.at[self.at(-d), pl.ds(0, n)]
            down = self.buf.at[self.at(d), pl.ds(n, n)]
        self.pending = (t.send(up, up, t.dev_z(1)), t.send(down, down, t.dev_z(-1)))


def together(chains, tick=None, lead=0):
    chains = list(chains)
    ended = object()
    for _ in range(lead):
        next(chains[0])
    while chains:
        for one in list(chains):
            if next(one, ended) is ended:
                chains.remove(one)
        if tick is not None:
            tick()


def attend(t, mem, w, beside):
    u = t.user
    copies = []
    out, into = t.new_out(), t.new_into()

    def double(ref):
        t.send(ref, ref, t.partner(), out, into)

    for dy, dx, dc in OTHERS:
        if dc == 0:
            y, x, c = t.shifted(dy, dx, dc)
            copies.append((dy, dx, t.send(mem.query.at[owned(y, x, c)[0]], mem.keys.at[t.me], (t.z, y, x, c), out)))
    mem.keys[t.me] = mem.query[u]
    double(mem.keys.at[t.me])
    beside()
    w.hop()
    for dy, dx, copy in reversed(copies):
        copy.wait_recv()
        y, x = lax.rem(t.y - dy + 4, 4), lax.rem(t.x - dx + 4, 4)
        double(mem.keys.at[(y * 4 + x) * 2 + t.c])
    t.await_all(mem.behaviors.at[pl.ds(0, 31)], mem.move_into)
    t.await_sent(mem.behaviors.at[pl.ds(0, 31)], mem.move_out)
    mem.own_behaviors.wait()
    t.await_all(mem.keys.at[pl.ds(0, 16)], into)
    t.await_sent(mem.keys.at[pl.ds(0, 31)], out)
    behaviors = mem.behaviors[...].reshape(WIDTH, QUARTER)
    s = dot(mem.keys[...].reshape(WIDTH, CANDS), behaviors, ((0,), (0,)))
    s = s * (1.0 / math.sqrt(WIDTH))
    at = lax.broadcasted_iota(jnp.int32, s.shape, 1) + t.quarter * QUARTER
    live = at < mem.lengths[u]
    s = jnp.where(live, s, -1e30)
    highest = jnp.max(s, axis=1, keepdims=True)
    e = jnp.where(live, jnp.exp(s - highest), 0.0)
    total = jnp.sum(e, axis=1, keepdims=True)
    some = total > 0.0
    total = jnp.where(some, total, 1.0)
    level = jnp.where(some, highest + jnp.log(total), -1e30)
    level = jnp.broadcast_to(level, (CANDS, 128))
    mem.levels[...] = level
    mem.level_tx[...] = level.T[:8]
    mem.level_copies = [
        t.send(mem.level_tx, mem.level_rx.at[i], dev) for i, (dev, _) in enumerate(owners(t))
    ]
    p = (e / total).astype(BF)
    for i in range(4):
        mem.means[i] = dot(p, mem.behaviors[pl.ds(8 * i, 8)].reshape(FEATURES, QUARTER), ((1,), (1,)))


def owners(t):
    x = t.x + 1 - 2 * lax.rem(t.x, 2)
    result = []
    for xx, c in ((x, 1 - t.c), (x, t.c), (t.x, 1 - t.c)):
        result.append(((t.z, t.y, xx, c), owned(t.y, xx, c)[1]))
    return result


def chain(t, h, mem, w):
    rows = pl.ds(h * ROWS, ROWS)
    copies = []
    for i, (dev, quarter) in enumerate(owners(t)):
        mem.mean_tx[h, i] = mem.means[quarter, rows, :].astype(BF)
        copies.append(t.send(mem.mean_tx.at[h, i], mem.mean_rx.at[h, i], dev))
    yield
    if h == 0:
        for copy in mem.level_copies:
            copy.wait_recv()
        levels = [mem.levels[...]]
        levels += [jnp.broadcast_to(mem.level_rx[i][:1], (128, CANDS)).T for i in range(3)]
        top = jnp.maximum(jnp.maximum(levels[0], levels[1]), jnp.maximum(levels[2], levels[3]))
        shares = [jnp.exp(level - top) for level in levels]
        scale = 1.0 / (shares[0] + shares[1] + shares[2] + shares[3])
        for i in range(4):
            mem.shares[i] = shares[i] * scale

    def share(i):
        return jnp.concatenate([mem.shares[i, rows, :]] * (FEATURES // 128), axis=1)

    total = mem.means[t.quarter, rows, :] * share(0)
    for i in (2, 1, 0):
        copies[i].wait_recv()
        total += mem.mean_rx[h, i].astype(F32) * share(i + 1)
    mem.pooled[h, t.quarter * USERS_HERE + t.user] = total.astype(BF)

    def pooled_slot(a, b):
        user, quarter = owned(*t.chip(a, b), t.c)
        return mem.pooled.at[h, quarter * USERS_HERE + user]

    yield from all_gather(
        t, pooled_slot, lambda n: mem.pooled.at[h, pl.ds(0, n)], MEAN_HALVES
    )
    if h == 0:
        w.wait()

    n = 256
    for i in range(TOKENS // n):
        acc = jnp.zeros((n, 2 * UNITS), F32)
        squares = jnp.zeros((n, 1), F32)
        for k in range(4):
            x = mem.pooled[h, pl.ds(USERS_HERE * k + 4 * i, 4)].reshape(n, FEATURES)
            acc += dot(x, mem.weights[pl.ds(2 * k, 2), :, pl.ds(0, 2 * UNITS)].reshape(FEATURES, 2 * UNITS))
            v = x.astype(F32)
            squares += jnp.sum(v * v, axis=1, keepdims=True)
        acc = acc * lax.rsqrt(squares * (1.0 / WIDTH) + 1e-6)
        gate, upward = acc[:, :UNITS], acc[:, UNITS:]
        value = gate / (1.0 + jnp.exp(-gate)) * upward
        mem.hidden[h, :, pl.ds(i * n, n)] = value.T.astype(BF)
    yield

    def outputs(core, group):
        parts = []
        for i in range(4):
            y = group + core * (i - group)
            x = i + core * (group - i)
            m = (y * 4 + x) * 2 + core
            at = pl.multiple_of(lax.rem(m, 4) * FEATS, FEATS)
            parts.append(mem.weights[m // 4, pl.ds(at, FEATS), pl.ds(2 * UNITS, UNITS)])
        return dot(jnp.concatenate(parts, axis=0), mem.hidden[h])

    total = yield from reduce_scatter(
        t,
        outputs,
        *(ref.at[h] for ref in mem.out_1),
        *(ref.at[h] for ref in mem.out_2),
    )
    mem.result[h] = total


class Memory:
    pass


def kernel(
    cand_in,
    behaviors_in,
    lengths,
    bilinear_in,
    gain,
    w_gate_in,
    w_up_in,
    w_down_in,
    out,
    behaviors,
    bilinear,
    raw_weights,
    weights,
    cands,
    query,
    keys,
    means,
    mean_tx,
    mean_rx,
    levels,
    level_tx,
    level_rx,
    shares,
    pooled,
    hidden,
    result,
    *rest,
):
    send_sem, recv_sem, in_sem = rest[-3:]
    t = Torus(send_sem, recv_sem)
    mem = Memory()
    mem.behaviors, mem.bilinear, mem.weights, mem.cands = behaviors, bilinear, weights, cands
    mem.query, mem.keys, mem.pooled, mem.hidden = query, keys, pooled, hidden
    mem.means, mem.mean_tx, mem.mean_rx, mem.shares = means, mean_tx, mean_rx, shares
    mem.levels, mem.level_tx, mem.level_rx = levels, level_tx, level_rx
    mem.lengths, mem.result = lengths, result
    mem.out_1, mem.out_2 = rest[0:5], rest[5:8]

    started = []

    def fetch(src, dst):
        copy = pltpu.make_async_copy(src, dst, in_sem.at[len(started)])
        copy.start()
        started.append(copy)
        return copy

    cand_copies = [
        fetch(
            cand_in.at[u],
            cands.at[u // CHUNK_USERS, t.me, :, pl.ds(u % CHUNK_USERS * CANDS, CANDS)],
        )
        for u in range(USERS_HERE)
    ]
    weight_copies = [
        fetch(w, raw_weights.at[i]) for i, w in enumerate((w_gate_in, w_up_in, w_down_in))
    ]
    bilinear_copy = fetch(bilinear_in, bilinear)

    def behaviors_of(y, x, core):
        user, quarter = owned(y, x, core)
        at = pl.multiple_of(quarter * QUARTER, QUARTER)
        return behaviors_in.at[user, :, pl.ds(at, QUARTER)]

    mem.own_behaviors = fetch(behaviors_of(t.y, t.x, t.c), behaviors.at[t.me])
    t.barrier()

    to_move = list(OTHERS)
    mem.move_out, mem.move_into = t.new_out(), t.new_into()

    def move_behaviors(count):
        for _ in range(min(count, len(to_move))):
            y, x, c = t.shifted(*to_move.pop(0))
            src, dst = behaviors_of(y, x, c), behaviors.at[t.me]
            t.send(src, dst, (t.z, y, x, c), mem.move_out, mem.move_into)

    def cand_slot(h):
        def slot(a, b):
            y, x = t.chip(a, b)
            return cands.at[h, (y * 4 + x) * 2 + t.c]

        return slot

    w = Weights(t, weights)
    for copy in cand_copies:
        copy.wait()
    gathers = [
        all_gather(t, cand_slot(h), lambda n, h=h: cands.at[h, pl.ds(0, n)], CAND_HALVES)
        for h in range(CHUNKS)
    ]
    for one in gathers:
        next(one)

    own_gain = gain[pl.ds(pl.multiple_of(t.z * UNITS, UNITS), UNITS)].reshape(1, UNITS)
    own_gain = jnp.broadcast_to(own_gain, (128, UNITS)).T
    own_gain = jnp.concatenate([own_gain, own_gain], axis=1)
    for i in range(3):
        weight_copies[i].wait()
        v = raw_weights[i].astype(F32)
        v = v * own_gain if i < 2 else v.T
        weights[t.z, :, pl.ds(i * UNITS, UNITS)] = v.astype(BF)
    w.hop()

    steps = iter(range(1, 99))

    def beside():
        step = next(steps)
        if step < len(MOVES):
            move_behaviors(MOVES[step])
        if step == SECOND_HOP:
            w.hop()

    move_behaviors(MOVES[0])
    together(gathers, beside)
    bilinear_copy.wait()
    for h in range(CHUNKS):
        q = dot(bilinear[...], cands[h].reshape(WIDTH, TOKENS)).astype(BF)
        for u in range(CHUNK_USERS):
            query[h * CHUNK_USERS + u] = q[:, u * CANDS : (u + 1) * CANDS]
    attend(t, mem, w, lambda: move_behaviors(len(to_move)))
    together([chain(t, h, mem, w) for h in range(CHUNKS)], w.late_hop, LEAD)
    for u in range(USERS_HERE):
        parts = [result[h, :, pl.ds(u // 2 * 128, 128)] for h in range(CHUNKS)]
        if u % 2 == 0:
            both = jnp.concatenate([part[:, :ROWS] for part in parts], axis=1)
        else:
            both = jnp.concatenate([part[:, ROWS:] for part in parts], axis=1)
        out[u] = both.astype(BF)
    t.finish()
    assert (t.outs, t.intos) == (N_OUT, N_INTO), (t.outs, t.intos)


def exchange_buffers(rows, piece, width):
    return (
        pltpu.VMEM((CHUNKS, 4, rows, width), BF),
        pltpu.VMEM((CHUNKS, 4, rows, width), BF),
        pltpu.VMEM((CHUNKS, 4, rows, width), F32),
        pltpu.VMEM((CHUNKS, 3, rows, width), BF),
        pltpu.VMEM((CHUNKS, 3, rows, width), BF),
        pltpu.VMEM((CHUNKS, 4, piece, width), F32),
        pltpu.VMEM((CHUNKS, 3, piece, width), BF),
        pltpu.VMEM((CHUNKS, 3, piece, width), BF),
    )


def shards(behaviors, candidates, lengths, bilinear, norm_gain, w_gate, w_up, w_down):
    vmem = pl.BlockSpec(memory_space=pltpu.VMEM)
    hbm = pl.BlockSpec(memory_space=pl.ANY)
    smem = pl.BlockSpec(memory_space=pltpu.SMEM)
    return pl.pallas_call(
        kernel,
        out_shape=jax.ShapeDtypeStruct(candidates.shape, BF),
        in_specs=[hbm, hbm, smem, hbm, vmem, hbm, hbm, hbm],
        out_specs=vmem,
        scratch_shapes=[
            pltpu.VMEM((32, FEATS, QUARTER), BF),
            pltpu.VMEM(bilinear.shape, BF),
            pltpu.VMEM((3, UNITS, UNITS), BF),
            pltpu.VMEM((8, UNITS, 3 * UNITS), BF),
            pltpu.VMEM((CHUNKS, 32, FEATS, TOKENS), BF),
            pltpu.VMEM((USERS_HERE, FEATS, CANDS), BF),
            pltpu.VMEM((32, FEATS, CANDS), BF),
            pltpu.VMEM((4, CANDS, FEATURES), F32),
            pltpu.VMEM((CHUNKS, 3, ROWS, FEATURES), BF),
            pltpu.VMEM((CHUNKS, 3, ROWS, FEATURES), BF),
            pltpu.VMEM((CANDS, 128), F32),
            pltpu.VMEM((8, CANDS), F32),
            pltpu.VMEM((3, 8, CANDS), F32),
            pltpu.VMEM((4, CANDS, 128), F32),
            pltpu.VMEM((CHUNKS, 4 * USERS_HERE, ROWS, FEATURES), BF),
            pltpu.VMEM((CHUNKS, UNITS, TOKENS), BF),
            pltpu.VMEM((CHUNKS, FEATS, TOKENS), F32),
            *exchange_buffers(256, FEATS, TOKENS),
            pltpu.SemaphoreType.DMA((N_OUT,)),
            pltpu.SemaphoreType.DMA((N_INTO,)),
            pltpu.SemaphoreType.DMA((16,)),
        ],
        compiler_params=pltpu.CompilerParams(
            collective_id=0, has_side_effects=True, vmem_limit_bytes=56 * 1024 * 1024
        ),
    )(
        candidates,
        behaviors,
        lengths,
        bilinear,
        norm_gain,
        w_gate,
        w_up,
        w_down,
    )


def solution(mesh):
    finer = Mesh(mesh.devices.reshape(mesh.shape["dp"], 4, 4, 2), ("dp", "mp_0", "mp_1", "mp_2"))
    return jax.shard_map(
        shards,
        mesh=finer,
        in_specs=(
            P("dp", MP, None),
            P("dp", MP, None),
            P("dp"),
            P(MP, None),
            P(),
            P("dp", MP),
            P("dp", MP),
            P(MP, "dp"),
        ),
        out_specs=P("dp", MP, None),
        check_vma=False,
    )
```

```python
import math

import jax
import jax.numpy as jnp
from jax import lax
from jax.experimental import pallas as pl
from jax.experimental.pallas import tpu as pltpu
from jax.sharding import Mesh
from jax.sharding import PartitionSpec as P

MP = ("mp_0", "mp_1", "mp_2")
MESH = pl.DeviceIdType.MESH
BF = jnp.bfloat16
F32 = jnp.float32
USERS_HERE = 8
CANDS = 128
WIDTH = 2048
BEHAVIORS = 1024
CHUNKS = 2
CHUNK_USERS = USERS_HERE // CHUNKS
TOKENS = CHUNK_USERS * CANDS
QUARTER = BEHAVIORS // 4
FEATURES = WIDTH // 4
ROWS = CANDS // CHUNKS
OTHERS = sorted(
    ((dy, dx, dc) for dy in range(4) for dx in range(4) for dc in range(2) if dy + dx + dc),
    key=lambda d: (-min(d[0], 4 - d[0]) - min(d[1], 4 - d[1]), d),
)
LEAD = 0
SECOND_HOP = 8
LAST_HOP = 4
MOVES = (6, 0, 4, 7, 7, 7)
CAND_HALVES = 32
MEAN_HALVES = 32
FEATS = 64
UNITS = 256
N_OUT, N_INTO = 43, 134


class Torus:
    def __init__(self, send_sem, recv_sem):
        self.z = lax.axis_index("dp")
        self.y = lax.axis_index("mp_0")
        self.x = lax.axis_index("mp_1")
        self.c = lax.axis_index("mp_2")
        self.a = self.x + self.c * (self.y - self.x)
        self.b = self.y + self.c * (self.x - self.y)
        self.me = (self.y * 4 + self.x) * 2 + self.c
        self.user, self.quarter = owned(self.y, self.x, self.c)
        self.send_sem, self.recv_sem = send_sem, recv_sem
        self.copies, self.ends = [], []
        self.outs = self.intos = 0

    def chip(self, a, b):
        return b + self.c * (a - b), a + self.c * (b - a)

    def shifted(self, dy, dx, dc):
        core = 1 - self.c if dc else self.c
        return lax.rem(self.y + dy, 4), lax.rem(self.x + dx, 4), core

    def dev_a(self, d):
        c = self.c
        return (self.z, lax.rem(self.y + c * d + 4, 4), lax.rem(self.x + (1 - c) * d + 4, 4), c)

    def dev_b(self, d):
        c = self.c
        return (self.z, lax.rem(self.y + (1 - c) * d + 4, 4), lax.rem(self.x + c * d + 4, 4), c)

    def dev_z(self, d):
        return (lax.rem(self.z + d + 8, 8), self.y, self.x, self.c)

    def partner(self):
        return (self.z, self.y, self.x, 1 - self.c)

    def new_out(self):
        self.outs += 1
        return self.outs - 1

    def new_into(self):
        self.intos += 1
        return self.intos - 1

    def copy(self, src, dst, dev, out, into):
        return pltpu.make_async_remote_copy(
            src_ref=src,
            dst_ref=dst,
            send_sem=self.send_sem.at[out],
            recv_sem=self.recv_sem.at[into],
            device_id=dev,
            device_id_type=MESH,
        )

    def send(self, src, dst, dev, out=None, into=None):
        alone = out is None
        out = self.new_out() if alone else out
        copy = self.copy(src, dst, dev, out, self.new_into() if into is None else into)
        copy.start()
        if alone:
            self.copies.append(copy)
        return copy

    def await_all(self, ref, into):
        self.copy(ref, ref, self.partner(), 0, into).wait_recv()

    def await_sent(self, ref, out):
        self.ends.append(self.copy(ref, ref, self.partner(), out, 0))

    def finish(self):
        for copy in self.copies + self.ends:
            copy.wait_send()

    def barrier(self):
        sem = pltpu.get_barrier_semaphore()
        peers = [self.dev_z(1), self.dev_z(-1)]
        peers += [(self.z, *self.shifted(*d)) for d in OTHERS]
        for dev in peers:
            pl.semaphore_signal(sem, inc=1, device_id=dev, device_id_type=MESH)
        return lambda: pl.semaphore_wait(sem, len(peers))


def owned(y, x, core):
    return y * 2 + x // 2, lax.rem(x, 2) * 2 + core


def all_gather(t, slot, blocks, halves=None):
    out, into = t.new_out(), t.new_into()

    def block(da, db):
        return slot(lax.rem(t.a + da + 4, 4), lax.rem(t.b + db + 4, 4))

    def whole(da, db, dev):
        ref = block(da, db)
        return t.send(ref, ref, dev, out)

    def double(da, db):
        ref = block(da, db)
        t.send(ref, ref, t.partner(), out, into)

    def part(da, db, h, dev):
        ref = block(da, db).at[pl.ds(h * halves, halves), :]
        return t.send(ref, ref, dev, out)

    far = (2, 1, -1) if halves is None else (1, -1)
    row = {d: whole(0, 0, t.dev_a(d)) for d in (1, -1, 2)}
    column = {(0, d): whole(0, 0, t.dev_b(d)) for d in far}
    double(0, 0)
    for q in (-1, 1, 2):
        yield
        row[q].wait_recv()
        for d in far:
            column[-q, d] = whole(-q, 0, t.dev_b(d))
        double(-q, 0)
    ends = {}
    for (q, d), copy in column.items():
        yield
        copy.wait_recv()
        if halves is not None:
            ends.setdefault(q, []).append(part(q, -d, 0 if d == 1 else 1, t.dev_b(d)))
        double(q, -d)
    for q, copies in ends.items():
        yield
        for copy in copies:
            copy.wait_recv()
        double(q, 2)
    yield
    t.await_all(blocks(16), into)
    t.await_sent(blocks(31), out)


def ring_sum(t, p, dev, terms, tx, rx):
    copies = []
    for i, d in enumerate((2, 1, -1)):
        tx[i] = terms[lax.rem(p + d + 4, 4)].astype(tx.dtype)
        copies.append(t.send(tx.at[i], rx.at[i], dev(d)))
    total = terms[p]
    for i in (1, 2, 0):
        yield
        copies[i].wait_recv()
        total += rx[i].astype(F32)
    return total


def reduce_scatter(t, term, twin_tx, twin_rx, terms, tx, rx, terms_2, tx_2, rx_2):
    other = 1 - t.c
    twins = []
    for d in (2, 1, -1, 0):
        g = lax.rem(t.a + d + 4, 4)
        twin_tx[g] = term(other, g).astype(twin_tx.dtype)
        twins.append(t.send(twin_tx.at[g], twin_rx.at[g], t.partner()))
    order = [lax.rem(t.b + d + 4, 4) for d in (2, 1, -1, 0)]
    for g in order:
        terms[g] = term(t.c, g)
    yield
    for copy, g in zip(twins, order):
        copy.wait_recv()
        terms[g] += twin_rx[g].astype(F32)
    total = yield from ring_sum(t, t.b, t.dev_b, terms, tx, rx)
    n = terms_2.shape[1]
    for i in range(4):
        terms_2[i] = total[i * n : (i + 1) * n]
    return (yield from ring_sum(t, t.a, t.dev_a, terms_2, tx_2, rx_2))


def dot(a, b, dims=((1,), (0,))):
    return lax.dot_general(a, b, (dims, ((), ())), preferred_element_type=F32)


class Weights:
    def __init__(self, t, buf):
        self.t, self.buf, self.hops, self.pending, self.ticks = t, buf, 0, (), 0

    def at(self, d):
        return lax.rem(self.t.z + d + 8, 8)

    def wait(self):
        for copy in self.pending:
            copy.wait_recv()
        self.pending = ()

    def late_hop(self):
        self.ticks += 1
        if self.ticks == LAST_HOP:
            self.hop()

    def hop(self):
        self.wait()
        t, d = self.t, self.hops
        self.hops += 1
        up, down = self.buf.at[self.at(-d)], self.buf.at[self.at(d)]
        if d == 3:
            n = self.buf.shape[1] // 2
            up = self.buf.at[self.at(-d), pl.ds(0, n)]
            down = self.buf.at[self.at(d), pl.ds(n, n)]
        self.pending = (t.send(up, up, t.dev_z(1)), t.send(down, down, t.dev_z(-1)))


def together(chains, tick=None, lead=0):
    chains = list(chains)
    ended = object()
    for _ in range(lead):
        next(chains[0])
    while chains:
        for one in list(chains):
            if next(one, ended) is ended:
                chains.remove(one)
        if tick is not None:
            tick()


def attend(t, mem, w, beside):
    u = t.user
    copies = []
    out, into = t.new_out(), t.new_into()

    def double(ref):
        t.send(ref, ref, t.partner(), out, into)

    for dy, dx, dc in OTHERS:
        if dc == 0:
            y, x, c = t.shifted(dy, dx, dc)
            copies.append((dy, dx, t.send(mem.query.at[owned(y, x, c)[0]], mem.keys.at[t.me], (t.z, y, x, c), out)))
    mem.keys[t.me] = mem.query[u]
    double(mem.keys.at[t.me])
    beside()
    w.hop()
    for dy, dx, copy in reversed(copies):
        copy.wait_recv()
        y, x = lax.rem(t.y - dy + 4, 4), lax.rem(t.x - dx + 4, 4)
        double(mem.keys.at[(y * 4 + x) * 2 + t.c])
    t.await_all(mem.behaviors.at[pl.ds(0, 31)], mem.move_into)
    t.await_sent(mem.behaviors.at[pl.ds(0, 31)], mem.move_out)
    mem.own_behaviors.wait()
    t.await_all(mem.keys.at[pl.ds(0, 16)], into)
    t.await_sent(mem.keys.at[pl.ds(0, 31)], out)
    behaviors = mem.behaviors[...].reshape(WIDTH, QUARTER)
    s = dot(mem.keys[...].reshape(WIDTH, CANDS), behaviors, ((0,), (0,)))
    s = s * (1.0 / math.sqrt(WIDTH))
    at = lax.broadcasted_iota(jnp.int32, s.shape, 1) + t.quarter * QUARTER
    live = at < mem.lengths[u]
    s = jnp.where(live, s, -1e30)
    highest = jnp.max(s, axis=1, keepdims=True)
    e = jnp.where(live, jnp.exp(s - highest), 0.0)
    total = jnp.sum(e, axis=1, keepdims=True)
    some = total > 0.0
    total = jnp.where(some, total, 1.0)
    level = jnp.where(some, highest + jnp.log(total), -1e30)
    level = jnp.broadcast_to(level, (CANDS, 128))
    mem.levels[...] = level
    mem.level_tx[...] = level.T[:8]
    mem.level_copies = [
        t.send(mem.level_tx, mem.level_rx.at[i], dev) for i, (dev, _) in enumerate(owners(t))
    ]
    p = (e / total).astype(BF)
    for i in range(4):
        mem.means[i] = dot(p, mem.behaviors[pl.ds(8 * i, 8)].reshape(FEATURES, QUARTER), ((1,), (1,)))


def owners(t):
    x = t.x + 1 - 2 * lax.rem(t.x, 2)
    result = []
    for xx, c in ((x, 1 - t.c), (x, t.c), (t.x, 1 - t.c)):
        result.append(((t.z, t.y, xx, c), owned(t.y, xx, c)[1]))
    return result


def chain(t, h, mem, w):
    rows = pl.ds(h * ROWS, ROWS)
    copies = []
    for i, (dev, quarter) in enumerate(owners(t)):
        mem.mean_tx[h, i] = mem.means[quarter, rows, :].astype(BF)
        copies.append(t.send(mem.mean_tx.at[h, i], mem.mean_rx.at[h, i], dev))
    yield
    if h == 0:
        for copy in mem.level_copies:
            copy.wait_recv()
        levels = [mem.levels[...]]
        levels += [jnp.broadcast_to(mem.level_rx[i][:1], (128, CANDS)).T for i in range(3)]
        top = jnp.maximum(jnp.maximum(levels[0], levels[1]), jnp.maximum(levels[2], levels[3]))
        shares = [jnp.exp(level - top) for level in levels]
        scale = 1.0 / (shares[0] + shares[1] + shares[2] + shares[3])
        for i in range(4):
            mem.shares[i] = shares[i] * scale

    def share(i):
        return jnp.concatenate([mem.shares[i, rows, :]] * (FEATURES // 128), axis=1)

    total = mem.means[t.quarter, rows, :] * share(0)
    for i in (2, 1, 0):
        copies[i].wait_recv()
        total += mem.mean_rx[h, i].astype(F32) * share(i + 1)
    mem.pooled[h, t.quarter * USERS_HERE + t.user] = total.astype(BF)

    def pooled_slot(a, b):
        user, quarter = owned(*t.chip(a, b), t.c)
        return mem.pooled.at[h, quarter * USERS_HERE + user]

    yield from all_gather(
        t, pooled_slot, lambda n: mem.pooled.at[h, pl.ds(0, n)], MEAN_HALVES
    )
    if h == 0:
        w.wait()

    n = 256
    for i in range(TOKENS // n):
        acc = jnp.zeros((n, 2 * UNITS), F32)
        squares = jnp.zeros((n, 1), F32)
        for k in range(4):
            x = mem.pooled[h, pl.ds(USERS_HERE * k + 4 * i, 4)].reshape(n, FEATURES)
            acc += dot(x, mem.weights[pl.ds(2 * k, 2), :, pl.ds(0, 2 * UNITS)].reshape(FEATURES, 2 * UNITS))
            v = x.astype(F32)
            squares += jnp.sum(v * v, axis=1, keepdims=True)
        acc = acc * lax.rsqrt(squares * (1.0 / WIDTH) + 1e-6)
        gate, upward = acc[:, :UNITS], acc[:, UNITS:]
        value = gate / (1.0 + jnp.exp(-gate)) * upward
        mem.hidden[h, :, pl.ds(i * n, n)] = value.T.astype(BF)
    yield

    def outputs(core, group):
        parts = []
        for i in range(4):
            y = group + core * (i - group)
            x = i + core * (group - i)
            m = (y * 4 + x) * 2 + core
            at = pl.multiple_of(lax.rem(m, 4) * FEATS, FEATS)
            parts.append(mem.weights[m // 4, pl.ds(at, FEATS), pl.ds(2 * UNITS, UNITS)])
        return dot(jnp.concatenate(parts, axis=0), mem.hidden[h])

    total = yield from reduce_scatter(
        t,
        outputs,
        *(ref.at[h] for ref in mem.out_1),
        *(ref.at[h] for ref in mem.out_2),
    )
    mem.result[h] = total


class Memory:
    pass


def kernel(
    cand_in,
    behaviors_in,
    lengths,
    bilinear_in,
    gain,
    w_gate_in,
    w_up_in,
    w_down_in,
    out,
    behaviors,
    bilinear,
    raw_weights,
    weights,
    cands,
    query,
    keys,
    means,
    mean_tx,
    mean_rx,
    levels,
    level_tx,
    level_rx,
    shares,
    pooled,
    hidden,
    result,
    *rest,
):
    send_sem, recv_sem, in_sem = rest[-3:]
    t = Torus(send_sem, recv_sem)
    entered = t.barrier()
    mem = Memory()
    mem.behaviors, mem.bilinear, mem.weights, mem.cands = behaviors, bilinear, weights, cands
    mem.query, mem.keys, mem.pooled, mem.hidden = query, keys, pooled, hidden
    mem.means, mem.mean_tx, mem.mean_rx, mem.shares = means, mean_tx, mean_rx, shares
    mem.levels, mem.level_tx, mem.level_rx = levels, level_tx, level_rx
    mem.lengths, mem.result = lengths, result
    mem.out_1, mem.out_2 = rest[0:5], rest[5:8]

    started = []

    def fetch(src, dst):
        copy = pltpu.make_async_copy(src, dst, in_sem.at[len(started)])
        copy.start()
        started.append(copy)
        return copy

    cand_copies = [
        fetch(
            cand_in.at[u],
            cands.at[u // CHUNK_USERS, t.me, :, pl.ds(u % CHUNK_USERS * CANDS, CANDS)],
        )
        for u in range(USERS_HERE)
    ]
    weight_copies = [
        fetch(w, raw_weights.at[i]) for i, w in enumerate((w_gate_in, w_up_in, w_down_in))
    ]
    bilinear_copy = fetch(bilinear_in, bilinear)

    def behaviors_of(y, x, core):
        user, quarter = owned(y, x, core)
        at = pl.multiple_of(quarter * QUARTER, QUARTER)
        return behaviors_in.at[user, :, pl.ds(at, QUARTER)]

    mem.own_behaviors = fetch(behaviors_of(t.y, t.x, t.c), behaviors.at[t.me])
    entered()

    to_move = list(OTHERS)
    mem.move_out, mem.move_into = t.new_out(), t.new_into()

    def move_behaviors(count):
        for _ in range(min(count, len(to_move))):
            y, x, c = t.shifted(*to_move.pop(0))
            src, dst = behaviors_of(y, x, c), behaviors.at[t.me]
            t.send(src, dst, (t.z, y, x, c), mem.move_out, mem.move_into)

    def cand_slot(h):
        def slot(a, b):
            y, x = t.chip(a, b)
            return cands.at[h, (y * 4 + x) * 2 + t.c]

        return slot

    w = Weights(t, weights)
    for copy in cand_copies:
        copy.wait()
    gathers = [
        all_gather(t, cand_slot(h), lambda n, h=h: cands.at[h, pl.ds(0, n)], CAND_HALVES)
        for h in range(CHUNKS)
    ]
    for one in gathers:
        next(one)

    own_gain = gain[pl.ds(pl.multiple_of(t.z * UNITS, UNITS), UNITS)].reshape(1, UNITS)
    own_gain = jnp.broadcast_to(own_gain, (128, UNITS)).T
    own_gain = jnp.concatenate([own_gain, own_gain], axis=1)
    for i in range(3):
        weight_copies[i].wait()
        v = raw_weights[i].astype(F32)
        v = v * own_gain if i < 2 else v.T
        weights[t.z, :, pl.ds(i * UNITS, UNITS)] = v.astype(BF)
    w.hop()

    steps = iter(range(1, 99))

    def beside():
        step = next(steps)
        if step < len(MOVES):
            move_behaviors(MOVES[step])
        if step == SECOND_HOP:
            w.hop()

    move_behaviors(MOVES[0])
    together(gathers, beside)
    bilinear_copy.wait()
    for h in range(CHUNKS):
        q = dot(bilinear[...], cands[h].reshape(WIDTH, TOKENS)).astype(BF)
        for u in range(CHUNK_USERS):
            query[h * CHUNK_USERS + u] = q[:, u * CANDS : (u + 1) * CANDS]
    attend(t, mem, w, lambda: move_behaviors(len(to_move)))
    together([chain(t, h, mem, w) for h in range(CHUNKS)], w.late_hop, LEAD)
    for u in range(USERS_HERE):
        parts = [result[h, :, pl.ds(u // 2 * 128, 128)] for h in range(CHUNKS)]
        if u % 2 == 0:
            both = jnp.concatenate([part[:, :ROWS] for part in parts], axis=1)
        else:
            both = jnp.concatenate([part[:, ROWS:] for part in parts], axis=1)
        out[u] = both.astype(BF)
    t.finish()
    assert (t.outs, t.intos) == (N_OUT, N_INTO), (t.outs, t.intos)


def exchange_buffers(rows, piece, width):
    return (
        pltpu.VMEM((CHUNKS, 4, rows, width), BF),
        pltpu.VMEM((CHUNKS, 4, rows, width), BF),
        pltpu.VMEM((CHUNKS, 4, rows, width), F32),
        pltpu.VMEM((CHUNKS, 3, rows, width), BF),
        pltpu.VMEM((CHUNKS, 3, rows, width), BF),
        pltpu.VMEM((CHUNKS, 4, piece, width), F32),
        pltpu.VMEM((CHUNKS, 3, piece, width), BF),
        pltpu.VMEM((CHUNKS, 3, piece, width), BF),
    )


def shards(behaviors, candidates, lengths, bilinear, norm_gain, w_gate, w_up, w_down):
    vmem = pl.BlockSpec(memory_space=pltpu.VMEM)
    hbm = pl.BlockSpec(memory_space=pl.ANY)
    smem = pl.BlockSpec(memory_space=pltpu.SMEM)
    return pl.pallas_call(
        kernel,
        out_shape=jax.ShapeDtypeStruct(candidates.shape, BF),
        in_specs=[hbm, hbm, smem, hbm, vmem, hbm, hbm, hbm],
        out_specs=vmem,
        scratch_shapes=[
            pltpu.VMEM((32, FEATS, QUARTER), BF),
            pltpu.VMEM(bilinear.shape, BF),
            pltpu.VMEM((3, UNITS, UNITS), BF),
            pltpu.VMEM((8, UNITS, 3 * UNITS), BF),
            pltpu.VMEM((CHUNKS, 32, FEATS, TOKENS), BF),
            pltpu.VMEM((USERS_HERE, FEATS, CANDS), BF),
            pltpu.VMEM((32, FEATS, CANDS), BF),
            pltpu.VMEM((4, CANDS, FEATURES), F32),
            pltpu.VMEM((CHUNKS, 3, ROWS, FEATURES), BF),
            pltpu.VMEM((CHUNKS, 3, ROWS, FEATURES), BF),
            pltpu.VMEM((CANDS, 128), F32),
            pltpu.VMEM((8, CANDS), F32),
            pltpu.VMEM((3, 8, CANDS), F32),
            pltpu.VMEM((4, CANDS, 128), F32),
            pltpu.VMEM((CHUNKS, 4 * USERS_HERE, ROWS, FEATURES), BF),
            pltpu.VMEM((CHUNKS, UNITS, TOKENS), BF),
            pltpu.VMEM((CHUNKS, FEATS, TOKENS), F32),
            *exchange_buffers(256, FEATS, TOKENS),
            pltpu.SemaphoreType.DMA((N_OUT,)),
            pltpu.SemaphoreType.DMA((N_INTO,)),
            pltpu.SemaphoreType.DMA((16,)),
        ],
        compiler_params=pltpu.CompilerParams(
            collective_id=0, has_side_effects=True, vmem_limit_bytes=56 * 1024 * 1024
        ),
    )(
        candidates,
        behaviors,
        lengths,
        bilinear,
        norm_gain,
        w_gate,
        w_up,
        w_down,
    )


def solution(mesh):
    finer = Mesh(mesh.devices.reshape(mesh.shape["dp"], 4, 4, 2), ("dp", "mp_0", "mp_1", "mp_2"))
    return jax.shard_map(
        shards,
        mesh=finer,
        in_specs=(
            P("dp", MP, None),
            P("dp", MP, None),
            P("dp"),
            P(MP, None),
            P(),
            P("dp", MP),
            P("dp", MP),
            P(MP, "dp"),
        ),
        out_specs=P("dp", MP, None),
        check_vma=False,
    )
```
